128 devices in a mesh: px: 16 (over y, z_hi, core), py: 8 (over x, z_lo).
Axes of the slice: x: 4, y: 4, z: 4 (z_hi: 2, z_lo: 2; z = z_hi * 2 + z_lo), core: 2. Of those that a mesh axis runs over, the one named last changes fastest.
Arguments:
- source: float32 [1024, 512, 128], P('px', 'py'), may hold values from -8 to 8
- layer_mass: float32 [128], replicated, may hold values from 0.5 to 4
- modes: float32 [128, 128], replicated, may hold values from -0.5 to 0.5
- mode_eigen: float32 [128], replicated, may hold values from 0.0002 to 1
Outputs:
- solution: float32 [1024, 512, 128], P('px', 'py')
The draws below stay inside these ranges and needn't reach their ends.
All inputs are finite; a program needn't handle non-finite values.
Results may differ from the reference program's by a relative error of at most 0.0014.
Values sent between devices are 32-bit elements; how exact they have to be, the bound alone decides.
No kernel may reach another device: no remote copies, remote signals or barrier semaphores. Data moves between devices by JAX's collectives and lax.ppermute only.
A program may use at most 64 MiB of HBM per device.

```python
import math
import jax
import jax.numpy as jnp
from jax import lax

NX = 1024
NY = 512
NZ = 128


def draw_source(key, part):
    first = jax.random.fold_in(key, 0)
    values = jax.random.normal(first, (NX, NY, NZ), jnp.float32)
    return jnp.clip(values, -8.0, 8.0).astype(jnp.float32)


def normal_values(stream_key, dims, scale, reach, kind=jnp.bfloat16):
    entries = scale * jax.random.normal(stream_key, dims, jnp.float32)
    return jnp.clip(entries, min=-reach, max=reach).astype(kind)


def setup_inputs(seed: int = 0) -> dict:
    arg_keys = jax.random.split(jax.random.key(seed), 5)
    return {
        "source": draw_source(jax.random.fold_in(arg_keys[4], 71), 0),
        "layer_mass": jnp.clip(jnp.exp(jax.random.uniform(arg_keys[1], (NZ,), jnp.float32, math.log(0.5), math.log(4.0))), 0.5, 4.0),
        "modes": normal_values(arg_keys[2], (NZ, NZ), NZ ** -0.5, 0.5, jnp.float32),
        "mode_eigen": jnp.clip(jnp.exp(jax.random.uniform(arg_keys[3], (NZ,), jnp.float32, math.log(0.0002), math.log(1.0))), 0.0002, 1.0),
    }


def cosine_table(length):
    rows = jnp.arange(length, dtype=jnp.float32)[:, None]
    cols = jnp.arange(length, dtype=jnp.float32)[None, :]
    scale = jnp.where(rows == 0.0, jnp.sqrt(1.0 / length), jnp.sqrt(2.0 / length)).astype(jnp.float32)
    return (scale * jnp.cos(jnp.pi * (cols + 0.5) * rows / length)).astype(jnp.float32)

def laplace_eigen(length):
    waves = jnp.arange(length, dtype=jnp.float32)
    return (2.0 - 2.0 * jnp.cos(jnp.pi * waves / length)).astype(jnp.float32)

def reference(source, layer_mass, modes, mode_eigen):
    high = lax.Precision.HIGHEST
    table_x = cosine_table(NX)
    table_y = cosine_table(NY)
    wave_x = laplace_eigen(NX)
    wave_y = laplace_eigen(NY)
    weighted = source * layer_mass
    modal_field = jnp.einsum('xyz,zk->kxy', weighted, modes, precision=high)

    def solve_mode(packed):
        planes, eigen_value = packed
        spectral = jnp.dot(jnp.dot(table_x, planes, precision=high), table_y.T, precision=high)
        scaled = spectral / (eigen_value + wave_x[:, None] + wave_y[None, :])
        return jnp.dot(jnp.dot(table_x.T, scaled, precision=high), table_y, precision=high)
    returned = lax.map(solve_mode, (modal_field, mode_eigen))
    return jnp.einsum('kxy,zk->xyz', returned, modes, precision=high)
```

```python
import jax
import jax.numpy as jnp
import numpy as np
from jax import lax
from jax.experimental import pallas as pl
from jax.experimental.pallas import tpu as pltpu
from jax.sharding import PartitionSpec as P

NX, NY, NZ = 1024, 512, 128
PX, PY = 16, 8
T = 64
H = T // 2
F32 = jnp.float32
BF16 = jnp.bfloat16
AXES = ("px", "py")


def np_split(table):
    table = np.asarray(table, np.float64)
    high = table.astype(np.float32).astype(jnp.bfloat16)
    low = (table - high.astype(np.float64)).astype(np.float32).astype(jnp.bfloat16)
    return high, low


def pair(table):
    return np.stack(np_split(table))


def sine_table():
    a = np.arange(1, T + 1)
    return np.sqrt(2.0 / (T + 1)) * np.sin(np.pi * np.outer(a, a) / (T + 1))


SINE = sine_table()
EDGE = SINE[:, 0]
LAM_T = 2.0 - 2.0 * np.cos(np.pi * np.arange(1, T + 1) / (T + 1))
ORDER_A = np.concatenate([np.arange(0, T, 2), np.arange(1, T, 2)])


def norm_row(length):
    return np.where(np.arange(length) == 0, np.sqrt(1.0 / length), np.sqrt(2.0 / length))


def tile_tables():
    ky = np.kron(np.eye(4), SINE)
    kx = np.stack([pair(np.kron(SINE[p::2, :H], np.eye(8))) for p in range(2)])
    kxt = np.stack([pair(np.kron(SINE[p::2, :H].T, np.eye(8))) for p in range(2)])
    edge_b = np.broadcast_to(EDGE[:, None], (T, NZ)).astype(np.float32)
    lam_b = np.broadcast_to(LAM_T[:, None], (T, NZ)).astype(np.float32)
    rows = np.stack([np.ones(8), (-1.0) ** np.arange(8)])
    ysel = np.concatenate([np.kron(np.eye(H), rows[s : s + 1]) for s in range(2)])
    return pair(ky), kx, kxt, np.stack([edge_b, lam_b]), ysel.astype(jnp.bfloat16)


def solve_tables():
    al, be = np.arange(NX), np.arange(NY)
    sx, sy = norm_row(NX), norm_row(NY)
    local = np.arange(T) + 0.5
    lines_x = np.stack([T * np.arange(PX) - 0.5, T * np.arange(PX) + T + 0.5])
    lines_y = np.stack([T * np.arange(PY) - 0.5, T * np.arange(PY) + T + 0.5])
    bkx = sx[:, None] * np.cos(np.pi * al[:, None] * lines_x.reshape(1, -1) / NX)
    bky = sy[:, None] * np.cos(np.pi * be[:, None] * lines_y.reshape(1, -1) / NY)
    bky = bky.reshape(NY, 2, 1, PY)
    bys = np.broadcast_to(bky, (NY, 2, PX, PY)).reshape(NY, 2 * PX * PY).T
    place = np.arange(NY) + 0.5
    cy = sy[:, None] * np.cos(np.pi * be[:, None] * place[None] / NY)
    cyl = np.einsum("bpy,cy->pcb", cy.reshape(NY, PY, T), SINE).reshape(NY, NY)
    phase = np.pi * al[:, None] * local[None] / NX
    m1 = (sx[:, None] * np.cos(phase)) @ SINE[:, ORDER_A]
    m2 = (sx[:, None] * np.sin(phase)) @ SINE[:, ORDER_A]
    turn = np.pi * np.arange(32)[:, None] * np.arange(PX)[None] / PX
    wide = lambda t: np.tile(np.repeat(t, PY, axis=1), (1, 2))
    turns = np.stack([wide(np.cos(turn)), wide(np.sin(turn))]).astype(np.float32)
    lam_x = (2.0 - 2.0 * np.cos(np.pi * al / NX)).astype(np.float32)[:, None]
    lam_y = (2.0 - 2.0 * np.cos(np.pi * be / NY)).astype(np.float32)[None]
    m12 = np.stack([pair(m1), pair(m2)])
    m12t = np.stack([pair(m1.T), pair(-m2.T)])
    return pair(bkx), pair(bkx.T), pair(bys), pair(cyl), m12, m12t, turns, lam_x, lam_y


def split(value):
    high = value.astype(BF16)
    return high, (value - high.astype(F32)).astype(BF16)


def dot(a, b, dims=(((1,), (0,)), ((), ()))):
    return lax.dot_general(a, b, dims, preferred_element_type=F32)


NT = (((1,), (1,)), ((), ()))


def dot3(a, b, dims=(((1,), (0,)), ((), ()))):
    return dot(a[0], b[0], dims) + dot(a[0], b[1], dims) + dot(a[1], b[0], dims)


def block_diag2(w):
    zero = jnp.zeros_like(w)
    top = jnp.concatenate([w, zero], axis=1)
    bottom = jnp.concatenate([zero, w], axis=1)
    return jnp.concatenate([top, bottom], axis=0)


def two(ref, *index):
    return ref[(*index, 0)], ref[(*index, 1)]


def forward_kernel(src, mass, modes, eig, ky, kx, rowtab, ysel, coef, edges, ybuf):
    w = split(mass[...] * modes[...])
    w = block_diag2(w[0]), block_diag2(w[1])
    kyp = two(ky)
    for g in range(8):
        near = src[4 * g : 4 * g + 4].reshape(4 * T, NZ)
        far = jnp.concatenate([src[63 - 4 * g - i] for i in range(4)], axis=0)
        folded = split(jnp.concatenate([near + far, near - far], axis=1))
        modal = split(dot3(folded, w))
        ybuf[4 * g : 4 * g + 4] = dot3(kyp, modal).reshape(4, T, 2 * NZ)
    eig_row = eig[...]
    across = [[None] * 8, [None] * 8]
    along = []
    for p in range(2):
        kxp = two(kx, p)
        acc_y = [None] * H
        for q in range(4):
            parts = [
                ybuf[:, 8 * o : 8 * o + 8, p * NZ : (p + 1) * NZ].reshape(8 * H, NZ)
                for o in (2 * q, 2 * q + 1)
            ]
            spec = dot3(kxp, split(jnp.concatenate(parts, axis=1)))
            for i in range(2):
                o = 2 * q + i
                block = spec[:, i * NZ : (i + 1) * NZ]
                coef[p, :, 8 * o : 8 * o + 8, :] = block.reshape(H, 8, NZ)
                base = eig_row + rowtab[1, 8 * o : 8 * o + 8, :]
                edge_b = rowtab[0, 8 * o : 8 * o + 8, :]
                acc_x = None
                for j in range(H):
                    a = 2 * j + p
                    v = block[8 * j : 8 * j + 8] / (base + float(LAM_T[a]))
                    vx = v * float(EDGE[a])
                    vy = v * edge_b
                    acc_x = vx if acc_x is None else acc_x + vx
                    acc_y[j] = vy if acc_y[j] is None else acc_y[j] + vy
                across[p][o] = acc_x
        along.append(jnp.concatenate(acc_y, axis=0))
    even = jnp.concatenate(across[0], axis=0)
    odd = jnp.concatenate(across[1], axis=0)
    sums = split(jnp.concatenate(along, axis=1))
    sel = ysel[...]
    ends = dot(sel, sums[0]) + dot(sel, sums[1])
    first = jnp.concatenate([ends[:H, :NZ], ends[:H, NZ:]], axis=0)
    last = jnp.concatenate([ends[H:, :NZ], ends[H:, NZ:]], axis=0)
    xs = jnp.concatenate([even + odd, even - odd], axis=0)
    ys = jnp.concatenate([first, last], axis=0)
    edges[:, 0, 0:NZ] = xs.T
    edges[:, 0, NZ : 2 * NZ] = ys.T


def interface_kernel(
    got, eig, bkx, bkxt, bys, cyl, m12, m12t, turns, lam_x, lam_y, out, xbuf
):
    mode = lax.axis_index("px") * PY + lax.axis_index("py")
    mu = eig[mode]
    lane = lax.broadcasted_iota(jnp.int32, (2 * PX, NZ), 1)
    low_half = lane < T
    xbuf[...] = got[:, 0, 0:NZ]
    tiles = []
    for q in range(4):
        rows = []
        for i in range(2):
            d = xbuf[pl.ds(2 * q + i, PX, stride=PY), :]
            swapped = pltpu.roll(d, T, 1)
            rows.append(jnp.concatenate([d, swapped] if i == 0 else [swapped, d], axis=0))
        tiles.append(jnp.where(low_half, rows[0], rows[1]))
    lines = jnp.concatenate(tiles, axis=1)
    cylp = two(cyl)
    t1 = split(dot3(split(lines), cylp))
    ends = got[:, 0, NZ : 2 * NZ].T
    ends = jnp.concatenate([ends[:T], ends[T:]], axis=1)
    endsp = split(ends)
    bysp = two(bys)
    cos_t = turns[0]
    sin_t = turns[1]
    shift = lam_y[...] + mu
    back_x = None
    back_y = None
    for c in range(4):
        rows = slice(256 * c, 256 * c + 256)
        m1 = m12[0, 0, rows], m12[0, 1, rows]
        m2 = m12[1, 0, rows], m12[1, 1, rows]
        z1 = dot3(m1, endsp).reshape(8, 32, 256) * cos_t[None]
        z2 = dot3(m2, endsp).reshape(8, 32, 256) * sin_t[None]
        z = split((z1 - z2).reshape(256, 256))
        spec = dot3((bkx[0, rows], bkx[1, rows]), t1) + dot3(z, bysp)
        u = split(spec / (shift + lam_x[rows]))
        bx = dot3((bkxt[0, :, rows], bkxt[1, :, rows]), u)
        back_x = bx if back_x is None else back_x + bx
        r = dot3(u, bysp, NT).reshape(8, 32, 256)
        r1 = split((r * cos_t[None]).reshape(256, 256))
        r2 = split((r * sin_t[None]).reshape(256, 256))
        by = dot3((m12t[0, 0, :, rows], m12t[0, 1, :, rows]), r1)
        by += dot3((m12t[1, 0, :, rows], m12t[1, 1, :, rows]), r2)
        back_y = by if back_y is None else back_y + by
    wx = dot3(split(back_x), cylp, NT)
    row = lax.broadcasted_iota(jnp.int32, (PX, NY), 0)
    before, after = lines[:PX], lines[PX:]
    wx0 = wx[:PX] + jnp.where(row == 0, before, pltpu.roll(after, 1, 0))
    wx1 = wx[PX:] + jnp.where(row == PX - 1, after, pltpu.roll(before, PX - 1, 0))
    low16 = low_half[:PX]
    for q in range(4):
        w0 = wx0[:, q * NZ : (q + 1) * NZ]
        w1 = wx1[:, q * NZ : (q + 1) * NZ]
        xbuf[pl.ds(2 * q, PX, stride=PY), :] = jnp.where(low16, w0, pltpu.roll(w1, T, 1))
        xbuf[pl.ds(2 * q + 1, PX, stride=PY), :] = jnp.where(low16, pltpu.roll(w0, T, 1), w1)
    out[:, 0, 0:NZ] = xbuf[...]
    col = lax.broadcasted_iota(jnp.int32, (T, NZ), 1) % PY
    before, after = ends[:, :NZ], ends[:, NZ:]
    wy0 = back_y[:, :NZ] + jnp.where(col == 0, before, pltpu.roll(after, 1, 1))
    wy1 = back_y[:, NZ:] + jnp.where(col == PY - 1, after, pltpu.roll(before, NZ - 1, 1))
    out[:, 0, NZ : 2 * NZ] = jnp.concatenate([wy0, wy1], axis=0).T


def backward_kernel(coef, got, modes, eig, ky, kxt, rowtab, dest, ybuf, qbuf):
    qbuf[0:NZ] = got[:, 0, 0:NZ].T
    qbuf[NZ : 2 * NZ] = got[:, 0, NZ : 2 * NZ].T
    eig_row = eig[...]
    sign = jnp.where(lax.broadcasted_iota(jnp.int32, (8, NZ), 0) % 2 == 0, 1.0, -1.0)
    w = split(modes[...].T)
    w = block_diag2(w[0]), block_diag2(w[1])
    for p in range(2):
        kxp = two(kxt, p)
        ends = [
            qbuf[NZ + p * H + j : NZ + p * H + j + 1] + sign * qbuf[NZ + T + p * H + j : NZ + T + p * H + j + 1]
            for j in range(H)
        ]
        for q in range(4):
            parts = []
            for o in (2 * q, 2 * q + 1):
                near = qbuf[8 * o : 8 * o + 8]
                far = qbuf[T + 8 * o : T + 8 * o + 8]
                line = near + far if p == 0 else near - far
                base = eig_row + rowtab[1, 8 * o : 8 * o + 8, :]
                edge_b = rowtab[0, 8 * o : 8 * o + 8, :]
                blocks = []
                for j in range(H):
                    a = 2 * j + p
                    r = coef[p, j, 8 * o : 8 * o + 8, :] + line * float(EDGE[a]) + ends[j] * edge_b
                    blocks.append(r / (base + float(LAM_T[a])))
                parts.append(jnp.concatenate(blocks, axis=0))
            back = dot3(kxp, split(jnp.concatenate(parts, axis=1)))
            for i in range(2):
                o = 2 * q + i
                ybuf[:, 8 * o : 8 * o + 8, p * NZ : (p + 1) * NZ] = back[
                    :, i * NZ : (i + 1) * NZ
                ].reshape(H, 8, NZ)
    kyp = two(ky)
    for g in range(8):
        block = split(ybuf[4 * g : 4 * g + 4].reshape(4 * T, 2 * NZ))
        modal = split(dot3(kyp, block))
        res = dot3(modal, w)
        near = res[:, :NZ]
        far = res[:, NZ:]
        dest[4 * g : 4 * g + 4] = (near + far).reshape(4, T, NZ)
        other = near - far
        for i in range(4):
            dest[63 - 4 * g - i] = other[T * i : T * i + T]


VMEM = pl.BlockSpec(memory_space=pltpu.VMEM)
SMEM = pl.BlockSpec(memory_space=pltpu.SMEM)
INTERPRET = False


def shards(source, layer_mass, modes, mode_eigen):
    ky, kx, kxt, rowtab, ysel = tile_tables()
    params = pltpu.CompilerParams(vmem_limit_bytes=48 * 1024 * 1024)
    coef, edges = pl.pallas_call(
        forward_kernel,
        out_shape=(
            jax.ShapeDtypeStruct((2, H, T, NZ), F32),
            jax.ShapeDtypeStruct((NZ, 1, 2 * NZ), F32),
        ),
        in_specs=[VMEM] * 8,
        out_specs=(VMEM, VMEM),
        scratch_shapes=[pltpu.VMEM((H, T, 2 * NZ), F32)],
        compiler_params=params,
        interpret=INTERPRET,
        name="forward",
    )(source, layer_mass[:, None], modes, mode_eigen[None], ky, kx, rowtab, ysel)
    edges = lax.all_to_all(edges, AXES, split_axis=0, concat_axis=0, tiled=True)
    values = pl.pallas_call(
        interface_kernel,
        out_shape=jax.ShapeDtypeStruct((NZ, 1, 2 * NZ), F32),
        in_specs=[VMEM, SMEM] + [VMEM] * 9,
        out_specs=VMEM,
        scratch_shapes=[pltpu.VMEM((NZ, NZ), F32)],
        compiler_params=params,
        interpret=INTERPRET,
        name="interface",
    )(edges, mode_eigen, *solve_tables())
    values = lax.all_to_all(values, AXES, split_axis=0, concat_axis=0, tiled=True)
    return pl.pallas_call(
        backward_kernel,
        out_shape=jax.ShapeDtypeStruct((T, T, NZ), F32),
        in_specs=[VMEM] * 7,
        out_specs=VMEM,
        scratch_shapes=[pltpu.VMEM((H, T, 2 * NZ), F32), pltpu.VMEM((2 * NZ, NZ), F32)],
        compiler_params=params,
        interpret=INTERPRET,
        name="backward",
    )(coef, values, modes, mode_eigen[None], ky, kxt, rowtab)


def solution(mesh):
    placed = (P("px", "py", None), P(), P(), P())
    return jax.shard_map(
        shards, mesh=mesh, in_specs=placed, out_specs=P("px", "py", None), check_vma=False
    )
```

```python
import jax
import jax.numpy as jnp
import numpy as np
from jax import lax
from jax.experimental import pallas as pl
from jax.experimental.pallas import tpu as pltpu
from jax.sharding import PartitionSpec as P

NX, NY, NZ = 1024, 512, 128
PX, PY = 16, 8
T = 64
H = T // 2
F32 = jnp.float32
BF16 = jnp.bfloat16
AXES = ("px", "py")


def np_split(table):
    table = np.asarray(table, np.float64)
    high = table.astype(np.float32).astype(jnp.bfloat16)
    low = (table - high.astype(np.float64)).astype(np.float32).astype(jnp.bfloat16)
    return high, low


def pair(table):
    return np.stack(np_split(table))


def sine_table():
    a = np.arange(1, T + 1)
    return np.sqrt(2.0 / (T + 1)) * np.sin(np.pi * np.outer(a, a) / (T + 1))


SINE = sine_table()
EDGE = SINE[:, 0]
LAM_T = 2.0 - 2.0 * np.cos(np.pi * np.arange(1, T + 1) / (T + 1))
ORDER_A = np.concatenate([np.arange(0, T, 2), np.arange(1, T, 2)])


def norm_row(length):
    return np.where(np.arange(length) == 0, np.sqrt(1.0 / length), np.sqrt(2.0 / length))


def tile_tables():
    rows = [SINE[p::2, :H] for p in range(2)] + [SINE[p::2, :H].T for p in range(2)]
    spread = np.concatenate([np.repeat(r, 8, axis=1) for r in rows])
    small = np.concatenate([spread, np.tile(SINE, (1, 4))]).astype(np.float32)
    edge_b = np.broadcast_to(EDGE[:, None], (T, NZ))
    lam_b = np.broadcast_to(LAM_T[:, None], (T, NZ))
    rowtab = np.concatenate([edge_b, lam_b]).astype(np.float32)
    signs = np.stack([np.ones(8), (-1.0) ** np.arange(8)])
    ysel = np.concatenate([np.kron(np.eye(H), signs[s : s + 1]) for s in range(2)])
    return small, rowtab, ysel.astype(jnp.bfloat16)


def solve_tables():
    al, be = np.arange(NX), np.arange(NY)
    sx, sy = norm_row(NX), norm_row(NY)
    by_parity = lambda n: np.concatenate([np.arange(0, n, 2), np.arange(1, n, 2)])
    al, be = by_parity(NX), by_parity(NY)
    sx, sy = sx[al], sy[be]
    local = np.arange(T) + 0.5
    lines_x = T * np.arange(PX) - 0.5
    lines_y = np.stack([T * np.arange(PY) - 0.5, T * np.arange(PY) + T + 0.5])
    bkx = sx[:, None] * np.cos(np.pi * al[:, None] * lines_x[None] / NX)
    bky = sy[:, None] * np.cos(np.pi * be[:, None] * lines_y.reshape(1, -1) / NY)
    bky = bky.reshape(NY, 2, 1, PY)
    bys = np.broadcast_to(bky, (NY, 2, PX // 2, PY)).reshape(NY, PX * PY).T
    place = np.arange(NY // 2) + 0.5
    cy = sy[:, None] * np.cos(np.pi * be[:, None] * place[None] / NY)
    cyl = np.einsum("bpy,cy->pcb", cy.reshape(NY, PY // 2, T), SINE).reshape(NY // 2, NY)
    cyl = np.stack([pair(cyl[:, : NY // 2]), pair(cyl[:, NY // 2 :])])
    phase = np.pi * al[:, None] * local[None] / NX
    m1 = (sx[:, None] * np.cos(phase)) @ SINE[:, ORDER_A]
    m2 = (sx[:, None] * np.sin(phase)) @ SINE[:, ORDER_A]
    m12 = np.concatenate(np_split(np.concatenate([m1, m2], axis=1)), axis=1)
    lam_x = 2.0 - 2.0 * np.cos(np.pi * al / NX)
    lam_h, lam_l = np_split(lam_x)
    rest = lam_x - lam_h.astype(np.float64) - lam_l.astype(np.float64)
    bkx_h, bkx_l = np_split(bkx)
    lams = np.stack([lam_h, lam_l, np_split(rest)[0]], axis=1)
    bkx_all = np.zeros((NX, 128), jnp.bfloat16)
    for i, part in enumerate((bkx_h, bkx_l, bkx_h, lams)):
        bkx_all[:, 16 * i : 16 * i + part.shape[1]] = part
    bkxt = np.stack([pair(bkx[512 * p : 512 * p + 512].T) for p in range(2)])
    px = np.arange(PX // 2)
    tz, tr = [], []
    for p in range(2):
        turn = np.pi * (2 * np.arange(16) + p)[:, None] * px[None] / PX
        wide = [np.tile(np.repeat(t, PY, axis=1), (1, 2)) for t in (np.cos(turn), -np.sin(turn))]
        tz.append(np.concatenate(wide, axis=1))
        tr += [np.tile(t.T, (1, 8)) for t in wide]
    tz = np.concatenate(tz).astype(np.float32)
    tr = np.stack(tr).astype(np.float32)
    lam_y = (2.0 - 2.0 * np.cos(np.pi * be / NY)).astype(np.float32)[None]
    return cyl, m12, bkx_all, bkxt, pair(bys), tz, tr, lam_y


def split(value):
    high = value.astype(BF16)
    return high, (value - high.astype(F32)).astype(BF16)


PLAIN = (((1,), (0,)), ((), ()))
NT = (((1,), (1,)), ((), ()))


def dot(a, b, dims=PLAIN):
    return lax.dot_general(a, b, dims, preferred_element_type=F32)


def dot3(a, b, dims=PLAIN):
    return dot(a[0], b[0], dims) + dot(a[0], b[1], dims) + dot(a[1], b[0], dims)


def block_diag2(w):
    zero = jnp.zeros_like(w)
    top = jnp.concatenate([w, zero], axis=1)
    bottom = jnp.concatenate([zero, w], axis=1)
    return jnp.concatenate([top, bottom], axis=0)


def two(ref, *index):
    return ref[(*index, 0)], ref[(*index, 1)]


def lanes(shape, axis):
    return lax.broadcasted_iota(jnp.int32, shape, axis)


def forward_kernel(*refs):
    src_in, mass_in, modes_in, eig_in, small_in, rowtab_in, ysel_in = refs[:7]
    tables_in = refs[7:15]
    coef, edges, ky, kxt, modes, eig, rowtab = refs[15:22]
    tables = refs[22:30]
    src, mass, small, ysel, kx, ybuf, sems = refs[30:]
    jobs = [(small_in, small), (mass_in, mass), (modes_in, modes)]
    for g in range(8):
        for lo in (4 * g, 60 - 4 * g):
            jobs.append((src_in.at[lo : lo + 4], src.at[lo : lo + 4]))
    jobs += [(eig_in, eig), (rowtab_in, rowtab), (ysel_in, ysel)]
    jobs += list(zip(tables_in, tables))
    copies = [pltpu.make_async_copy(a, b, sems.at[i]) for i, (a, b) in enumerate(jobs)]
    for copy in copies:
        copy.start()
    for copy in copies[:3]:
        copy.wait()
    row_block = lanes((T, 4 * T), 1) // T
    for i in range(4):
        part = split(jnp.where(row_block == i, small[4 * H : 4 * H + T, :], 0.0))
        for h in range(2):
            ky[h, T * i : T * i + T, :] = part[h]
    diagonal = lanes((8, 8 * H), 1) % 8 == lanes((8, 8 * H), 0)
    for t in range(4):
        spread = [
            jnp.where(diagonal, small[H * t + j : H * t + j + 1, :], 0.0) for j in range(H)
        ]
        part = split(jnp.concatenate(spread, axis=0))
        for h in range(2):
            if t < 2:
                kx[t, h] = part[h]
            else:
                kxt[t - 2, h] = part[h]
    mass_col = jnp.broadcast_to(mass[...], (NZ, NZ)).T
    w = split(mass_col * modes[...])
    w = block_diag2(w[0]), block_diag2(w[1])
    kyp = two(ky)
    for g in range(8):
        for copy in copies[3 + 2 * g : 5 + 2 * g]:
            copy.wait()
        near = src[4 * g : 4 * g + 4].reshape(4 * T, NZ)
        far = jnp.concatenate([src[63 - 4 * g - i] for i in range(4)], axis=0)
        folded = split(jnp.concatenate([near + far, near - far], axis=1))
        modal = split(dot3(folded, w))
        ybuf[4 * g : 4 * g + 4] = dot3(kyp, modal).reshape(4, T, 2 * NZ)
    for copy in copies[19:22]:
        copy.wait()
    eig_row = eig[...]
    across = [[None] * 8, [None] * 8]
    along = []
    for p in range(2):
        kxp = two(kx, p)
        acc_y = [None] * H
        for q in range(4):
            parts = [
                ybuf[:, 8 * o : 8 * o + 8, p * NZ : (p + 1) * NZ].reshape(8 * H, NZ)
                for o in (2 * q, 2 * q + 1)
            ]
            spec = dot3(kxp, split(jnp.concatenate(parts, axis=1)))
            for i in range(2):
                o = 2 * q + i
                block = spec[:, i * NZ : (i + 1) * NZ]
                coef[p, :, 8 * o : 8 * o + 8, :] = block.reshape(H, 8, NZ)
                base = eig_row + rowtab[T + 8 * o : T + 8 * o + 8, :]
                edge_b = rowtab[8 * o : 8 * o + 8, :]
                acc_x = None
                for j in range(H):
                    a = 2 * j + p
                    v = block[8 * j : 8 * j + 8] / (base + float(LAM_T[a]))
                    vx = v * float(EDGE[a])
                    vy = v * edge_b
                    acc_x = vx if acc_x is None else acc_x + vx
                    acc_y[j] = vy if acc_y[j] is None else acc_y[j] + vy
                across[p][o] = acc_x
        along.append(jnp.concatenate(acc_y, axis=0))
    even = jnp.concatenate(across[0], axis=0)
    odd = jnp.concatenate(across[1], axis=0)
    sums = split(jnp.concatenate(along, axis=1))
    sel = ysel[...]
    ends = dot(sel, sums[0]) + dot(sel, sums[1])
    first = jnp.concatenate([ends[:H, :NZ], ends[:H, NZ:]], axis=0)
    last = jnp.concatenate([ends[H:, :NZ], ends[H:, NZ:]], axis=0)
    xs = jnp.concatenate([even + odd, even - odd], axis=0)
    ys = jnp.concatenate([first, last], axis=0)
    edges[:, 0, 0:NZ] = xs.T
    edges[:, 0, NZ : 2 * NZ] = ys.T
    for copy in copies[22:]:
        copy.wait()


def turned(m):
    return jnp.concatenate([m[PY * (PX - 1 - i) : PY * (PX - i)] for i in range(PX)], axis=0)


def swap(m):
    return pltpu.roll(m, T, 1)


def interface_kernel(got, eig, cyl, m12, bkx, bkxt, bys, tz, tr, lam_y, out, xbuf):
    mode = lax.axis_index("px") * PY + lax.axis_index("py")
    mu = jnp.sum(jnp.where(lanes((1, NZ), 1) == mode, eig[...], 0.0), axis=1, keepdims=True)
    lane = lanes((NZ, NZ), 1)
    low = lane < T
    low32 = low[: 2 * PX]
    low16 = low[:PX]
    low64 = low[:T]
    sign_b = jnp.where(lanes((2 * PX, NZ), 1) % 2 == 0, 1.0, -1.0)
    sign_a = jnp.where(lanes((T, NZ), 1) % T < H, 1.0, -1.0)
    gx = got[:, 0, 0:NZ]
    gy = got[:, 0, NZ : 2 * NZ]

    mirror = swap(turned(gx))
    xbuf[...] = jnp.where(low, gx + mirror, swap(gx - mirror))
    tiles = []
    for q in range(4):
        rows = []
        for i in range(2):
            d = xbuf[pl.ds(2 * q + i, PX, stride=PY), :]
            other = swap(d)
            rows.append(jnp.concatenate([d, other] if i == 0 else [other, d], axis=0))
        tiles.append(jnp.where(low32, rows[0], rows[1]))
    flipped = [sign_b * swap(tiles[3 - q]) for q in range(2)]
    line_e = jnp.concatenate([tiles[q] + flipped[q] for q in range(2)], axis=1)
    line_o = jnp.concatenate([tiles[q] - flipped[q] for q in range(2)], axis=1)
    t1 = jnp.concatenate(
        [dot3(split(line_e), two(cyl, 0)), dot3(split(line_o), two(cyl, 1))], axis=1
    )
    t1h, t1l = split(t1)

    back = turned(gy)[:T]
    part_e = gy[:T] + sign_a * back
    part_o = gy[:T] - sign_a * back
    ends = jnp.concatenate(
        [jnp.where(low64, part_e, swap(part_o)), jnp.where(low64, swap(part_e), part_o)], axis=0
    ).T
    by_h, by_l = two(bys)
    by_lh = jnp.concatenate([by_l, by_h], axis=0)
    shift = lam_y[...] + mu
    back_x, back_y = [], []
    for p in range(2):
        e = split(ends[T * p : T * p + T])
        eh, el = block_diag2(e[0]), block_diag2(e[1])
        ehh = jnp.concatenate([eh, eh], axis=0)
        th, tl = t1h[PX * p : PX * p + PX], t1l[PX * p : PX * p + PX]
        pad = jnp.zeros((NZ - 3 * PX, NY), BF16)
        weights = jnp.concatenate([by_h, th, th, tl, pad], axis=0)
        sum_x = sum_y = None
        for c in range(2):
            rows = slice(512 * p + 256 * c, 512 * p + 256 * c + 256)
            m = m12[rows]
            zz = dot(m, ehh) + dot(m[:, :NZ], el)
            zz = (zz.reshape(16, 16, 256) * tz[16 * p : 16 * p + 16][None]).reshape(256, 256)
            zh, zl = split(zz[:, :NZ] + zz[:, NZ:])
            bk = bkx[rows]
            spec = dot(jnp.concatenate([zh, bk], axis=1), weights)
            spec += dot(jnp.concatenate([zh, zl], axis=1), by_lh)
            lams = bk[:, 48:51].astype(F32)
            lam = (lams[:, 2:3] + lams[:, 1:2]) + lams[:, 0:1]
            u = split(spec / (shift + lam))
            cols = slice(256 * c, 256 * c + 256)
            bx = dot3((bkxt[p, 0, :, cols], bkxt[p, 1, :, cols]), u)
            r = dot3((by_h, by_l), u, NT)
            turns = [jnp.concatenate([tr[2 * p + i]] * 2, axis=1) for i in range(2)]
            rh, rl = split(jnp.concatenate([r * turns[0], r * turns[1]], axis=0))
            wide = dot(rh, m)
            by = wide[:, :NZ] + wide[:, NZ:] + dot(rl, m[:, :NZ])
            sum_x = bx if c == 0 else sum_x + bx
            sum_y = by if c == 0 else sum_y + by
        back_x.append(sum_x)
        back_y.append(sum_y[:NZ] + swap(sum_y[NZ:]))

    bx = jnp.concatenate(back_x, axis=0)
    we = dot3(split(bx[:, : NY // 2]), two(cyl, 0), NT)
    wo = dot3(split(bx[:, NY // 2 :]), two(cyl, 1), NT)
    near = we + wo
    far = we - wo
    for q in range(4):
        if q < 2:
            t = near[:, q * NZ : (q + 1) * NZ]
        else:
            t = swap(sign_b * far[:, (3 - q) * NZ : (4 - q) * NZ])
        s0 = t[:PX] + t[PX:]
        s1 = t[:PX] - t[PX:]
        xbuf[pl.ds(2 * q, PX, stride=PY), :] = jnp.where(low16, s0, swap(s1))
        xbuf[pl.ds(2 * q + 1, PX, stride=PY), :] = jnp.where(low16, swap(s0), s1)
    w = xbuf[...]
    other = swap(gx)
    own = jnp.where(
        low,
        jnp.concatenate([gx[:PY], other[:-PY]], axis=0),
        jnp.concatenate([other[PY:], gx[-PY:]], axis=0),
    )
    out[:, 0, 0:NZ] = jnp.where(low, w, turned(w)) + own

    near = back_y[0] + back_y[1]
    far = back_y[0] - back_y[1]
    near = jnp.where(low64, near[:T], swap(near[T:]))
    far = sign_a * jnp.where(low64, far[:T], swap(far[T:]))
    w = jnp.concatenate([near, turned(jnp.concatenate([far, far], axis=0))[:T]], axis=0)
    row = lanes((NZ, NZ), 0) % PY
    other = swap(gy)
    own = jnp.where(
        low,
        jnp.where(row == 0, gy, pltpu.roll(other, 1, 0)),
        jnp.where(row == PY - 1, gy, pltpu.roll(other, NZ - 1, 0)),
    )
    out[:, 0, NZ : 2 * NZ] = w + own


def backward_kernel(coef, got, modes, eig, ky, kxt, rowtab, dest, ybuf, qbuf, obuf, sems):
    qbuf[0:NZ] = got[:, 0, 0:NZ].T
    qbuf[NZ : 2 * NZ] = got[:, 0, NZ : 2 * NZ].T
    eig_row = eig[...]
    sign = jnp.where(lanes((8, NZ), 0) % 2 == 0, 1.0, -1.0)
    w = split(modes[...].T)
    w = block_diag2(w[0]), block_diag2(w[1])
    for p in range(2):
        kxp = two(kxt, p)
        ends = []
        for j in range(H):
            at = NZ + p * H + j
            ends.append(qbuf[at : at + 1] + sign * qbuf[at + T : at + T + 1])
        for q in range(4):
            parts = []
            for o in (2 * q, 2 * q + 1):
                near = qbuf[8 * o : 8 * o + 8]
                far = qbuf[T + 8 * o : T + 8 * o + 8]
                line = near + far if p == 0 else near - far
                base = eig_row + rowtab[T + 8 * o : T + 8 * o + 8, :]
                edge_b = rowtab[8 * o : 8 * o + 8, :]
                blocks = []
                for j in range(H):
                    a = 2 * j + p
                    r = coef[p, j, 8 * o : 8 * o + 8, :] + line * float(EDGE[a]) + ends[j] * edge_b
                    blocks.append(r / (base + float(LAM_T[a])))
                parts.append(jnp.concatenate(blocks, axis=0))
            back = dot3(kxp, split(jnp.concatenate(parts, axis=1)))
            for i in range(2):
                o = 2 * q + i
                ybuf[:, 8 * o : 8 * o + 8, p * NZ : (p + 1) * NZ] = back[
                    :, i * NZ : (i + 1) * NZ
                ].reshape(H, 8, NZ)
    kyp = two(ky)
    copies = []
    for g in range(8):
        block = split(ybuf[4 * g : 4 * g + 4].reshape(4 * T, 2 * NZ))
        modal = split(dot3(kyp, block))
        res = dot3(modal, w)
        near = res[:, :NZ]
        far = res[:, NZ:]
        obuf[4 * g : 4 * g + 4] = (near + far).reshape(4, T, NZ)
        other = near - far
        for i in range(4):
            obuf[63 - 4 * g - i] = other[T * i : T * i + T]
        for i, lo in enumerate((4 * g, 60 - 4 * g)):
            copies.append(
                pltpu.make_async_copy(
                    obuf.at[lo : lo + 4], dest.at[lo : lo + 4], sems.at[2 * g + i]
                )
            )
            copies[-1].start()
    for copy in copies:
        copy.wait()


VMEM = pl.BlockSpec(memory_space=pltpu.VMEM)
HBM = pl.BlockSpec(memory_space=pltpu.HBM)
INTERPRET = False


def like(array):
    return jax.ShapeDtypeStruct(array.shape, array.dtype)


def shards(source, layer_mass, modes, mode_eigen):
    small, rowtab, ysel = tile_tables()
    tables = solve_tables()
    params = pltpu.CompilerParams(vmem_limit_bytes=40 * 1024 * 1024)
    eig = mode_eigen[None]
    mass = layer_mass[None]
    edge_shape = jax.ShapeDtypeStruct((NZ, 1, 2 * NZ), F32)
    kron = (2, 8 * H, 8 * H)
    made = pl.pallas_call(
        forward_kernel,
        out_shape=(
            jax.ShapeDtypeStruct((2, H, T, NZ), F32),
            edge_shape,
            jax.ShapeDtypeStruct(kron, BF16),
            jax.ShapeDtypeStruct((2, *kron), BF16),
            like(modes),
            like(eig),
            like(rowtab),
            *[like(t) for t in tables],
        ),
        in_specs=[HBM] * (7 + len(tables)),
        out_specs=[VMEM] * (7 + len(tables)),
        scratch_shapes=[
            pltpu.VMEM((T, T, NZ), F32),
            pltpu.VMEM((1, NZ), F32),
            pltpu.VMEM(small.shape, F32),
            pltpu.VMEM(ysel.shape, BF16),
            pltpu.VMEM((2, *kron), BF16),
            pltpu.VMEM((H, T, 2 * NZ), F32),
            pltpu.SemaphoreType.DMA((22 + len(tables),)),
        ],
        compiler_params=params,
        interpret=INTERPRET,
        name="forward",
    )(source, mass, modes, eig, small, rowtab, ysel, *tables)
    coef, edges, ky, kxt, modes, eig, rowtab = made[:7]
    edges = lax.all_to_all(edges, AXES, split_axis=0, concat_axis=0, tiled=True)
    values = pl.pallas_call(
        interface_kernel,
        out_shape=edge_shape,
        in_specs=[VMEM] * (2 + len(tables)),
        out_specs=VMEM,
        scratch_shapes=[pltpu.VMEM((NZ, NZ), F32)],
        compiler_params=params,
        interpret=INTERPRET,
        name="interface",
    )(edges, eig, *made[7:])
    values = lax.all_to_all(values, AXES, split_axis=0, concat_axis=0, tiled=True)
    return pl.pallas_call(
        backward_kernel,
        out_shape=jax.ShapeDtypeStruct((T, T, NZ), F32),
        in_specs=[VMEM] * 7,
        out_specs=HBM,
        scratch_shapes=[
            pltpu.VMEM((H, T, 2 * NZ), F32),
            pltpu.VMEM((2 * NZ, NZ), F32),
            pltpu.VMEM((T, T, NZ), F32),
            pltpu.SemaphoreType.DMA((16,)),
        ],
        compiler_params=params,
        interpret=INTERPRET,
        name="backward",
    )(coef, values, modes, eig, ky, kxt, rowtab)


def solution(mesh):
    placed = (P("px", "py", None), P(), P(), P())
    return jax.shard_map(
        shards, mesh=mesh, in_specs=placed, out_specs=P("px", "py", None), check_vma=False
    )
```

```python
import jax
import jax.numpy as jnp
import numpy as np
from jax import lax
from jax.experimental import pallas as pl
from jax.experimental.pallas import tpu as pltpu
from jax.sharding import PartitionSpec as P

NX, NY, NZ = 1024, 512, 128
PX, PY = 16, 8
T = 64
H = T // 2
F32 = jnp.float32
BF16 = jnp.bfloat16
AXES = ("px", "py")


def np_split(table):
    table = np.asarray(table, np.float64)
    high = table.astype(np.float32).astype(jnp.bfloat16)
    low = (table - high.astype(np.float64)).astype(np.float32).astype(jnp.bfloat16)
    return high, low


def pair(table):
    return np.stack(np_split(table))


def sine_table():
    a = np.arange(1, T + 1)
    return np.sqrt(2.0 / (T + 1)) * np.sin(np.pi * np.outer(a, a) / (T + 1))


SINE = sine_table()
EDGE = SINE[:, 0]
LAM_T = 2.0 - 2.0 * np.cos(np.pi * np.arange(1, T + 1) / (T + 1))
ORDER_A = np.concatenate([np.arange(0, T, 2), np.arange(1, T, 2)])


def norm_row(length):
    return np.where(np.arange(length) == 0, np.sqrt(1.0 / length), np.sqrt(2.0 / length))


def tile_tables():
    rows = [SINE[p::2, :H] for p in range(2)] + [SINE[p::2, :H].T for p in range(2)]
    spread = np.concatenate([np.repeat(r, 8, axis=1) for r in rows])
    small = np.concatenate([spread, np.tile(SINE, (1, 4))]).astype(np.float32)
    edge_b = np.broadcast_to(EDGE[:, None], (T, NZ))
    lam_b = np.broadcast_to(LAM_T[:, None], (T, NZ))
    rowtab = np.concatenate([edge_b, lam_b]).astype(np.float32)
    signs = np.stack([np.ones(8), (-1.0) ** np.arange(8)])
    ysel = np.concatenate([np.kron(np.eye(H), signs[s : s + 1]) for s in range(2)])
    return small, rowtab, ysel.astype(jnp.bfloat16)


def solve_tables():
    al, be = np.arange(NX), np.arange(NY)
    sx, sy = norm_row(NX), norm_row(NY)
    by_parity = lambda n: np.concatenate([np.arange(0, n, 2), np.arange(1, n, 2)])
    al, be = by_parity(NX), by_parity(NY)
    sx, sy = sx[al], sy[be]
    local = np.arange(T) + 0.5
    lines_x = T * np.arange(PX) - 0.5
    lines_y = np.stack([T * np.arange(PY) - 0.5, T * np.arange(PY) + T + 0.5])
    bkx = sx[:, None] * np.cos(np.pi * al[:, None] * lines_x[None] / NX)
    bky = sy[:, None] * np.cos(np.pi * be[:, None] * lines_y.reshape(1, -1) / NY)
    bky = bky.reshape(NY, 2, 1, PY)
    bys = np.broadcast_to(bky, (NY, 2, PX // 2, PY)).reshape(NY, PX * PY).T
    place = np.arange(NY // 2) + 0.5
    cy = sy[:, None] * np.cos(np.pi * be[:, None] * place[None] / NY)
    cyl = np.einsum("bpy,cy->pcb", cy.reshape(NY, PY // 2, T), SINE).reshape(NY // 2, NY)
    cyl = np.stack([pair(cyl[:, : NY // 2]), pair(cyl[:, NY // 2 :])])
    phase = np.pi * al[:, None] * local[None] / NX
    m1 = (sx[:, None] * np.cos(phase)) @ SINE[:, ORDER_A]
    m2 = (sx[:, None] * np.sin(phase)) @ SINE[:, ORDER_A]
    m12 = np.concatenate(np_split(np.concatenate([m1, m2], axis=1)), axis=1)
    lam_x = 2.0 - 2.0 * np.cos(np.pi * al / NX)
    lam_h, lam_l = np_split(lam_x)
    rest = lam_x - lam_h.astype(np.float64) - lam_l.astype(np.float64)
    bkx_h, bkx_l = np_split(bkx)
    lams = np.stack([lam_h, lam_l, np_split(rest)[0]], axis=1)
    bkx_all = np.zeros((NX, 128), jnp.bfloat16)
    for i, part in enumerate((bkx_h, bkx_l, bkx_h, lams)):
        bkx_all[:, 16 * i : 16 * i + part.shape[1]] = part
    bkxt = np.stack([pair(bkx[512 * p : 512 * p + 512].T) for p in range(2)])
    px = np.arange(PX // 2)
    tz, tr = [], []
    for p in range(2):
        turn = np.pi * (2 * np.arange(16) + p)[:, None] * px[None] / PX
        wide = [np.tile(np.repeat(t, PY, axis=1), (1, 2)) for t in (np.cos(turn), -np.sin(turn))]
        tz.append(np.concatenate(wide, axis=1))
        tr += [np.tile(t.T, (1, 8)) for t in wide]
    tz = np.concatenate(tz).astype(np.float32)
    tr = np.stack(tr).astype(np.float32)
    lam_y = (2.0 - 2.0 * np.cos(np.pi * be / NY)).astype(np.float32)[None]
    return cyl, m12, bkx_all, bkxt, pair(bys), tz, tr, lam_y


def split(value):
    high = value.astype(BF16)
    return high, (value - high.astype(F32)).astype(BF16)


PLAIN = (((1,), (0,)), ((), ()))
NT = (((1,), (1,)), ((), ()))


def dot(a, b, dims=PLAIN):
    return lax.dot_general(a, b, dims, preferred_element_type=F32)


def dot3(a, b, dims=PLAIN):
    return dot(a[0], b[0], dims) + dot(a[0], b[1], dims) + dot(a[1], b[0], dims)


def block_diag2(w):
    zero = jnp.zeros_like(w)
    top = jnp.concatenate([w, zero], axis=1)
    bottom = jnp.concatenate([zero, w], axis=1)
    return jnp.concatenate([top, bottom], axis=0)


def two(ref, *index):
    return ref[(*index, 0)], ref[(*index, 1)]


def lanes(shape, axis):
    return lax.broadcasted_iota(jnp.int32, shape, axis)


def forward_kernel(*refs):
    src_in, mass_in, modes_in, eig_in, small_in, rowtab_in, ysel_in = refs[:7]
    tables_in = refs[7:15]
    coef, edges, ky, kxt, modes, eig, rowtab = refs[15:22]
    tables = refs[22:30]
    src, mass, small, ysel, kx, ybuf, sems = refs[30:]
    jobs = [(small_in, small), (mass_in, mass), (modes_in, modes)]
    for g in range(8):
        for lo in (4 * g, 60 - 4 * g):
            jobs.append((src_in.at[lo : lo + 4], src.at[lo : lo + 4]))
    jobs += [(eig_in, eig), (rowtab_in, rowtab), (ysel_in, ysel)]
    jobs += list(zip(tables_in, tables))
    copies = [pltpu.make_async_copy(a, b, sems.at[i]) for i, (a, b) in enumerate(jobs)]
    for copy in copies:
        copy.start()
    for copy in copies[:3]:
        copy.wait()
    row_block = lanes((T, 4 * T), 1) // T
    for i in range(4):
        part = split(jnp.where(row_block == i, small[4 * H : 4 * H + T, :], 0.0))
        for h in range(2):
            ky[h, T * i : T * i + T, :] = part[h]
    diagonal = lanes((8, 8 * H), 1) % 8 == lanes((8, 8 * H), 0)
    for t in range(4):
        spread = [
            jnp.where(diagonal, small[H * t + j : H * t + j + 1, :], 0.0) for j in range(H)
        ]
        part = split(jnp.concatenate(spread, axis=0))
        for h in range(2):
            if t < 2:
                kx[t, h] = part[h]
            else:
                kxt[t - 2, h] = part[h]
    mass_col = jnp.broadcast_to(mass[...], (NZ, NZ)).T
    w = split(mass_col * modes[...])
    w = block_diag2(w[0]), block_diag2(w[1])
    kyp = two(ky)
    for g in range(8):
        for copy in copies[3 + 2 * g : 5 + 2 * g]:
            copy.wait()
        near = src[4 * g : 4 * g + 4].reshape(4 * T, NZ)
        far = jnp.concatenate([src[63 - 4 * g - i] for i in range(4)], axis=0)
        folded = split(jnp.concatenate([near + far, near - far], axis=1))
        modal = split(dot3(folded, w))
        ybuf[4 * g : 4 * g + 4] = dot3(kyp, modal).reshape(4, T, 2 * NZ)
    for copy in copies[19:22]:
        copy.wait()
    eig_row = eig[...]
    across = [[None] * 8, [None] * 8]
    along = []
    for p in range(2):
        kxp = two(kx, p)
        acc_y = [None] * H
        for q in range(4):
            parts = [
                ybuf[:, 8 * o : 8 * o + 8, p * NZ : (p + 1) * NZ].reshape(8 * H, NZ)
                for o in (2 * q, 2 * q + 1)
            ]
            spec = dot3(kxp, split(jnp.concatenate(parts, axis=1)))
            for i in range(2):
                o = 2 * q + i
                block = spec[:, i * NZ : (i + 1) * NZ]
                coef[p, :, 8 * o : 8 * o + 8, :] = block.reshape(H, 8, NZ)
                base = eig_row + rowtab[T + 8 * o : T + 8 * o + 8, :]
                edge_b = rowtab[8 * o : 8 * o + 8, :]
                acc_x = None
                for j in range(H):
                    a = 2 * j + p
                    v = block[8 * j : 8 * j + 8] / (base + float(LAM_T[a]))
                    vx = v * float(EDGE[a])
                    vy = v * edge_b
                    acc_x = vx if acc_x is None else acc_x + vx
                    acc_y[j] = vy if acc_y[j] is None else acc_y[j] + vy
                across[p][o] = acc_x
        along.append(jnp.concatenate(acc_y, axis=0))
    even = jnp.concatenate(across[0], axis=0)
    odd = jnp.concatenate(across[1], axis=0)
    sums = split(jnp.concatenate(along, axis=1))
    sel = ysel[...]
    ends = dot(sel, sums[0]) + dot(sel, sums[1])
    first = jnp.concatenate([ends[:H, :NZ], ends[:H, NZ:]], axis=0)
    last = jnp.concatenate([ends[H:, :NZ], ends[H:, NZ:]], axis=0)
    xs = jnp.concatenate([even + odd, even - odd], axis=0)
    ys = jnp.concatenate([first, last], axis=0)
    edges[:, 0, 0:NZ] = xs.T
    edges[:, 0, NZ : 2 * NZ] = ys.T
    for copy in copies[22:]:
        copy.wait()


def turned(m):
    return jnp.concatenate([m[PY * (PX - 1 - i) : PY * (PX - i)] for i in range(PX)], axis=0)


def swap(m):
    return pltpu.roll(m, T, 1)


def interface_kernel(got, eig, cyl, m12, bkx, bkxt, bys, tz, tr, lam_y, out, xbuf):
    mode = lax.axis_index("px") * PY + lax.axis_index("py")
    mu = jnp.sum(jnp.where(lanes((1, NZ), 1) == mode, eig[...], 0.0), axis=1, keepdims=True)
    lane = lanes((NZ, NZ), 1)
    low = lane < T
    low32 = low[: 2 * PX]
    low16 = low[:PX]
    low64 = low[:T]
    sign_b = jnp.where(lanes((2 * PX, NZ), 1) % 2 == 0, 1.0, -1.0)
    sign_a = jnp.where(lanes((T, NZ), 1) % T < H, 1.0, -1.0)
    gx = got[:, 0, 0:NZ]
    gy = got[:, 0, NZ : 2 * NZ]

    mirror = swap(turned(gx))
    xbuf[...] = jnp.where(low, gx + mirror, swap(gx - mirror))
    tiles = []
    for q in range(4):
        rows = []
        for i in range(2):
            d = xbuf[pl.ds(2 * q + i, PX, stride=PY), :]
            other = swap(d)
            rows.append(jnp.concatenate([d, other] if i == 0 else [other, d], axis=0))
        tiles.append(jnp.where(low32, rows[0], rows[1]))
    flipped = [sign_b * swap(tiles[3 - q]) for q in range(2)]
    line_e = jnp.concatenate([tiles[q] + flipped[q] for q in range(2)], axis=1)
    line_o = jnp.concatenate([tiles[q] - flipped[q] for q in range(2)], axis=1)
    t1 = jnp.concatenate(
        [dot3(split(line_e), two(cyl, 0)), dot3(split(line_o), two(cyl, 1))], axis=1
    )
    t1h, t1l = split(t1)

    back = turned(gy)[:T]
    part_e = gy[:T] + sign_a * back
    part_o = gy[:T] - sign_a * back
    ends = jnp.concatenate(
        [jnp.where(low64, part_e, swap(part_o)), jnp.where(low64, swap(part_e), part_o)], axis=0
    ).T
    by_h, by_l = two(bys)
    by_lh = jnp.concatenate([by_l, by_h], axis=0)
    shift = lam_y[...] + mu
    back_x, back_y = [], []
    for p in range(2):
        e = split(ends[T * p : T * p + T])
        eh, el = block_diag2(e[0]), block_diag2(e[1])
        ehh = jnp.concatenate([eh, eh], axis=0)
        th, tl = t1h[PX * p : PX * p + PX], t1l[PX * p : PX * p + PX]
        pad = jnp.zeros((NZ - 3 * PX, NY), BF16)
        weights = jnp.concatenate([by_h, th, th, tl, pad], axis=0)
        sum_x = sum_y = None
        for c in range(2):
            rows = slice(512 * p + 256 * c, 512 * p + 256 * c + 256)
            m = m12[rows]
            zz = dot(m, ehh) + dot(m[:, :NZ], el)
            zz = (zz.reshape(16, 16, 256) * tz[16 * p : 16 * p + 16][None]).reshape(256, 256)
            zh, zl = split(zz[:, :NZ] + zz[:, NZ:])
            bk = bkx[rows]
            spec = dot(jnp.concatenate([zh, bk], axis=1), weights)
            spec += dot(jnp.concatenate([zh, zl], axis=1), by_lh)
            lams = bk[:, 48:51].astype(F32)
            lam = (lams[:, 2:3] + lams[:, 1:2]) + lams[:, 0:1]
            u = split(spec / (shift + lam))
            cols = slice(256 * c, 256 * c + 256)
            bx = dot3((bkxt[p, 0, :, cols], bkxt[p, 1, :, cols]), u)
            r = dot3((by_h, by_l), u, NT)
            turns = [jnp.concatenate([tr[2 * p + i]] * 2, axis=1) for i in range(2)]
            rh, rl = split(jnp.concatenate([r * turns[0], r * turns[1]], axis=0))
            wide = dot(rh, m)
            by = wide[:, :NZ] + wide[:, NZ:] + dot(rl, m[:, :NZ])
            sum_x = bx if c == 0 else sum_x + bx
            sum_y = by if c == 0 else sum_y + by
        back_x.append(sum_x)
        back_y.append(sum_y[:NZ] + swap(sum_y[NZ:]))

    bx = jnp.concatenate(back_x, axis=0)
    we = dot3(split(bx[:, : NY // 2]), two(cyl, 0), NT)
    wo = dot3(split(bx[:, NY // 2 :]), two(cyl, 1), NT)
    near = we + wo
    far = we - wo
    for q in range(4):
        if q < 2:
            t = near[:, q * NZ : (q + 1) * NZ]
        else:
            t = swap(sign_b * far[:, (3 - q) * NZ : (4 - q) * NZ])
        s0 = t[:PX] + t[PX:]
        s1 = t[:PX] - t[PX:]
        xbuf[pl.ds(2 * q, PX, stride=PY), :] = jnp.where(low16, s0, swap(s1))
        xbuf[pl.ds(2 * q + 1, PX, stride=PY), :] = jnp.where(low16, swap(s0), s1)
    w = xbuf[...]
    other = swap(gx)
    own = jnp.where(
        low,
        jnp.concatenate([gx[:PY], other[:-PY]], axis=0),
        jnp.concatenate([other[PY:], gx[-PY:]], axis=0),
    )
    out[:, 0, 0:NZ] = jnp.where(low, w, turned(w)) + own

    near = back_y[0] + back_y[1]
    far = back_y[0] - back_y[1]
    near = jnp.where(low64, near[:T], swap(near[T:]))
    far = sign_a * jnp.where(low64, far[:T], swap(far[T:]))
    w = jnp.concatenate([near, turned(jnp.concatenate([far, far], axis=0))[:T]], axis=0)
    row = lanes((NZ, NZ), 0) % PY
    other = swap(gy)
    own = jnp.where(
        low,
        jnp.where(row == 0, gy, pltpu.roll(other, 1, 0)),
        jnp.where(row == PY - 1, gy, pltpu.roll(other, NZ - 1, 0)),
    )
    out[:, 0, NZ : 2 * NZ] = w + own


def backward_kernel(coef, got, modes, eig, ky, kxt, rowtab, dest, ybuf, qbuf, obuf, sems):
    qbuf[0:NZ] = got[:, 0, 0:NZ].T
    qbuf[NZ : 2 * NZ] = got[:, 0, NZ : 2 * NZ].T
    eig_row = eig[...]
    sign = jnp.where(lanes((8, NZ), 0) % 2 == 0, 1.0, -1.0)
    w = split(modes[...].T)
    w = block_diag2(w[0]), block_diag2(w[1])
    for p in range(2):
        kxp = two(kxt, p)
        ends = []
        for j in range(H):
            at = NZ + p * H + j
            ends.append(qbuf[at : at + 1] + sign * qbuf[at + T : at + T + 1])
        for q in range(4):
            parts = []
            for o in (2 * q, 2 * q + 1):
                near = qbuf[8 * o : 8 * o + 8]
                far = qbuf[T + 8 * o : T + 8 * o + 8]
                line = near + far if p == 0 else near - far
                base = eig_row + rowtab[T + 8 * o : T + 8 * o + 8, :]
                edge_b = rowtab[8 * o : 8 * o + 8, :]
                blocks = []
                for j in range(H):
                    a = 2 * j + p
                    r = coef[p, j, 8 * o : 8 * o + 8, :] + line * float(EDGE[a]) + ends[j] * edge_b
                    blocks.append(r / (base + float(LAM_T[a])))
                parts.append(jnp.concatenate(blocks, axis=0))
            back = dot3(kxp, split(jnp.concatenate(parts, axis=1)))
            for i in range(2):
                o = 2 * q + i
                ybuf[:, 8 * o : 8 * o + 8, p * NZ : (p + 1) * NZ] = back[
                    :, i * NZ : (i + 1) * NZ
                ].reshape(H, 8, NZ)
    kyp = two(ky)
    copies = []
    for g in range(8):
        block = split(ybuf[4 * g : 4 * g + 4].reshape(4 * T, 2 * NZ))
        modal = split(dot3(kyp, block))
        res = dot3(modal, w)
        near = res[:, :NZ]
        far = res[:, NZ:]
        obuf[4 * g : 4 * g + 4] = (near + far).reshape(4, T, NZ)
        other = near - far
        for i in range(4):
            obuf[63 - 4 * g - i] = other[T * i : T * i + T]
        for i, lo in enumerate((4 * g, 60 - 4 * g)):
            copies.append(
                pltpu.make_async_copy(
                    obuf.at[lo : lo + 4], dest.at[lo : lo + 4], sems.at[2 * g + i]
                )
            )
            copies[-1].start()
    for copy in copies:
        copy.wait()


VMEM = pl.BlockSpec(memory_space=pltpu.VMEM)
HBM = pl.BlockSpec(memory_space=pltpu.HBM)
INTERPRET = False


def like(array):
    return jax.ShapeDtypeStruct(array.shape, array.dtype)


def shards(source, layer_mass, modes, mode_eigen):
    small, rowtab, ysel = tile_tables()
    tables = solve_tables()
    params = pltpu.CompilerParams(vmem_limit_bytes=40 * 1024 * 1024)
    eig = mode_eigen[None]
    mass = layer_mass[None]
    edge_shape = jax.ShapeDtypeStruct((NZ, 1, 2 * NZ), F32)
    kron = (2, 8 * H, 8 * H)
    operands = [
        pltpu.with_memory_space_constraint(jnp.asarray(v), pltpu.HBM)
        for v in (source, mass, modes, eig, small, rowtab, ysel, *tables)
    ]
    made = pl.pallas_call(
        forward_kernel,
        out_shape=(
            jax.ShapeDtypeStruct((2, H, T, NZ), F32),
            edge_shape,
            jax.ShapeDtypeStruct(kron, BF16),
            jax.ShapeDtypeStruct((2, *kron), BF16),
            like(modes),
            like(eig),
            like(rowtab),
            *[like(t) for t in tables],
        ),
        in_specs=[HBM] * (7 + len(tables)),
        out_specs=[VMEM] * (7 + len(tables)),
        scratch_shapes=[
            pltpu.VMEM((T, T, NZ), F32),
            pltpu.VMEM((1, NZ), F32),
            pltpu.VMEM(small.shape, F32),
            pltpu.VMEM(ysel.shape, BF16),
            pltpu.VMEM((2, *kron), BF16),
            pltpu.VMEM((H, T, 2 * NZ), F32),
            pltpu.SemaphoreType.DMA((22 + len(tables),)),
        ],
        compiler_params=params,
        interpret=INTERPRET,
        name="forward",
    )(*operands)
    coef, edges, ky, kxt, modes, eig, rowtab = made[:7]
    edges = lax.all_to_all(edges, AXES, split_axis=0, concat_axis=0, tiled=True)
    values = pl.pallas_call(
        interface_kernel,
        out_shape=edge_shape,
        in_specs=[VMEM] * (2 + len(tables)),
        out_specs=VMEM,
        scratch_shapes=[pltpu.VMEM((NZ, NZ), F32)],
        compiler_params=params,
        interpret=INTERPRET,
        name="interface",
    )(edges, eig, *made[7:])
    values = lax.all_to_all(values, AXES, split_axis=0, concat_axis=0, tiled=True)
    return pl.pallas_call(
        backward_kernel,
        out_shape=jax.ShapeDtypeStruct((T, T, NZ), F32),
        in_specs=[VMEM] * 7,
        out_specs=HBM,
        scratch_shapes=[
            pltpu.VMEM((H, T, 2 * NZ), F32),
            pltpu.VMEM((2 * NZ, NZ), F32),
            pltpu.VMEM((T, T, NZ), F32),
            pltpu.SemaphoreType.DMA((16,)),
        ],
        compiler_params=params,
        interpret=INTERPRET,
        name="backward",
    )(coef, values, modes, eig, ky, kxt, rowtab)


def solution(mesh):
    placed = (P("px", "py", None), P(), P(), P())
    return jax.shard_map(
        shards, mesh=mesh, in_specs=placed, out_specs=P("px", "py", None), check_vma=False
    )
```

```python
import jax
import jax.numpy as jnp
import numpy as np
from jax import lax
from jax.experimental import pallas as pl
from jax.experimental.pallas import tpu as pltpu
from jax.sharding import PartitionSpec as P

NX, NY, NZ = 1024, 512, 128
PX, PY = 16, 8
T = 64
H = T // 2
F32 = jnp.float32
BF16 = jnp.bfloat16
AXES = ("px", "py")


def np_split(table):
    table = np.asarray(table, np.float64)
    high = table.astype(np.float32).astype(jnp.bfloat16)
    low = (table - high.astype(np.float64)).astype(np.float32).astype(jnp.bfloat16)
    return high, low


def pair(table):
    return np.stack(np_split(table))


def sine_table():
    a = np.arange(1, T + 1)
    return np.sqrt(2.0 / (T + 1)) * np.sin(np.pi * np.outer(a, a) / (T + 1))


SINE = sine_table()
EDGE = SINE[:, 0]
LAM_T = 2.0 - 2.0 * np.cos(np.pi * np.arange(1, T + 1) / (T + 1))
ORDER_A = np.concatenate([np.arange(0, T, 2), np.arange(1, T, 2)])


def norm_row(length):
    return np.where(np.arange(length) == 0, np.sqrt(1.0 / length), np.sqrt(2.0 / length))


def tile_tables():
    rows = [SINE[p::2, :H] for p in range(2)] + [SINE[p::2, :H].T for p in range(2)]
    spread = np.concatenate([np.repeat(r, 8, axis=1) for r in rows])
    small = np.concatenate([spread, np.tile(SINE, (1, 4))]).astype(np.float32)
    edge_b = np.broadcast_to(EDGE[:, None], (T, NZ))
    lam_b = np.broadcast_to(LAM_T[:, None], (T, NZ))
    rowtab = np.concatenate([edge_b, lam_b], axis=1).astype(np.float32)
    signs = np.stack([np.ones(8), (-1.0) ** np.arange(8)])
    ysel = np.concatenate([np.kron(np.eye(H), signs[s : s + 1]) for s in range(2)])
    return small, rowtab, ysel.astype(jnp.bfloat16)


def solve_tables():
    al, be = np.arange(NX), np.arange(NY)
    sx, sy = norm_row(NX), norm_row(NY)
    by_parity = lambda n: np.concatenate([np.arange(0, n, 2), np.arange(1, n, 2)])
    al, be = by_parity(NX), by_parity(NY)
    sx, sy = sx[al], sy[be]
    local = np.arange(T) + 0.5
    lines_x = T * np.arange(PX) - 0.5
    lines_y = np.stack([T * np.arange(PY) - 0.5, T * np.arange(PY) + T + 0.5])
    bkx = sx[:, None] * np.cos(np.pi * al[:, None] * lines_x[None] / NX)
    bky = sy[:, None] * np.cos(np.pi * be[:, None] * lines_y.reshape(1, -1) / NY)
    bky = bky.reshape(NY, 2, 1, PY)
    bys = np.broadcast_to(bky, (NY, 2, PX // 2, PY)).reshape(NY, PX * PY).T
    place = np.arange(NY // 2) + 0.5
    cy = sy[:, None] * np.cos(np.pi * be[:, None] * place[None] / NY)
    cyl = np.einsum("bpy,cy->pcb", cy.reshape(NY, PY // 2, T), SINE).reshape(NY // 2, NY)
    cyl = np.stack([pair(cyl[:, : NY // 2]), pair(cyl[:, NY // 2 :])])
    phase = np.pi * al[:, None] * local[None] / NX
    m1 = (sx[:, None] * np.cos(phase)) @ SINE[:, ORDER_A]
    m2 = (sx[:, None] * np.sin(phase)) @ SINE[:, ORDER_A]
    m12 = np.concatenate(np_split(np.concatenate([m1, m2], axis=1)), axis=1)
    lam_x = 2.0 - 2.0 * np.cos(np.pi * al / NX)
    lam_h, lam_l = np_split(lam_x)
    rest = lam_x - lam_h.astype(np.float64) - lam_l.astype(np.float64)
    bkx_h, bkx_l = np_split(bkx)
    lams = np.stack([lam_h, lam_l, np_split(rest)[0]], axis=1)
    bkx_all = np.zeros((NX, 128), jnp.bfloat16)
    for i, part in enumerate((bkx_h, bkx_l, bkx_h, lams)):
        bkx_all[:, 16 * i : 16 * i + part.shape[1]] = part
    bkxt = np.stack([pair(bkx[512 * p : 512 * p + 512].T) for p in range(2)])
    px = np.arange(PX // 2)
    tz, tr = [], []
    for p in range(2):
        turn = np.pi * (2 * np.arange(16) + p)[:, None] * px[None] / PX
        wide = [np.tile(np.repeat(t, PY, axis=1), (1, 2)) for t in (np.cos(turn), -np.sin(turn))]
        tz.append(np.concatenate(wide, axis=1))
        tr += [np.tile(t.T, (1, 8)) for t in wide]
    tz = np.concatenate(tz).astype(np.float32)
    tr = np.stack(tr).astype(np.float32)
    lam_y = (2.0 - 2.0 * np.cos(np.pi * be / NY)).astype(np.float32)[None]
    bys = pair(bys)
    bys = np.concatenate([bys[:, :, :256], bys[:, :, 256:]], axis=1)
    bkx_all = bkx_all.reshape(2, 2, 256, 128)
    bkx_all = np.concatenate([bkx_all[:, 0], bkx_all[:, 1]], axis=2)
    bkxt = bkxt.reshape(2, 2, 16, 2, 256).transpose(0, 1, 3, 2, 4)
    tr = np.stack([np.concatenate([tr[2 * p], tr[2 * p + 1]], axis=1) for p in range(2)])
    small, rowtab, ysel = tile_tables()
    lam_y = np.concatenate([lam_y.reshape(2, 256), np.zeros((6, 256), np.float32)])
    flat = lambda parts: np.concatenate([t.reshape(-1, 256) for t in parts])
    return flat([small, rowtab, tz, tr, lam_y]), flat([cyl, m12, bkx_all, bys, bkxt, ysel])


SMALL, ROWTAB, TZ, TR, LAM_Y = 0, 192, 256, 288, 544
CYL, M12, BKX, BYS, BKXT, YSEL = 0, 1024, 2048, 2560, 3072, 3200


def split(value):
    high = value.astype(BF16)
    return high, (value - high.astype(F32)).astype(BF16)


PLAIN = (((1,), (0,)), ((), ()))
NT = (((1,), (1,)), ((), ()))


def dot(a, b, dims=PLAIN):
    return lax.dot_general(a, b, dims, preferred_element_type=F32)


def dot3(a, b, dims=PLAIN):
    return dot(a[0], b[0], dims) + dot(a[0], b[1], dims) + dot(a[1], b[0], dims)


def block_diag2(w):
    zero = jnp.zeros_like(w)
    top = jnp.concatenate([w, zero], axis=1)
    bottom = jnp.concatenate([zero, w], axis=1)
    return jnp.concatenate([top, bottom], axis=0)


def two(ref, *index):
    return ref[(*index, 0)], ref[(*index, 1)]


def lanes(shape, axis):
    return lax.broadcasted_iota(jnp.int32, shape, axis)


def forward_kernel(
    src_in, mass_in, modes_in, eig_in, tab_in, wide_in,
    coef, recip, edges, ky, kxt, modes, eig, tab, wide,
    src, mass, kx, ybuf, sems,
):
    jobs = [(tab_in, tab), (eig_in, eig), (mass_in, mass), (modes_in, modes)]
    for lo, hi in ((0, 16), (48, 64), (16, 48)):
        jobs.append((src_in.at[lo:hi], src.at[lo:hi]))
    jobs.append((wide_in, wide))
    copies = [pltpu.make_async_copy(a, b, sems.at[i]) for i, (a, b) in enumerate(jobs)]
    for copy in copies:
        copy.start()
    copies[0].wait()
    row_block = lanes((T, 4 * T), 1) // T
    for i in range(4):
        part = split(jnp.where(row_block == i, tab[4 * H : 4 * H + T, :], 0.0))
        for h in range(2):
            ky[h, T * i : T * i + T, :] = part[h]
    diagonal = lanes((8, 8 * H), 1) % 8 == lanes((8, 8 * H), 0)
    for t in range(4):
        spread = [jnp.where(diagonal, tab[H * t + j : H * t + j + 1, :], 0.0) for j in range(H)]
        part = split(jnp.concatenate(spread, axis=0))
        for h in range(2):
            if t < 2:
                kx[t, h] = part[h]
            else:
                kxt[t - 2, h] = part[h]
    copies[1].wait()
    eig_row = eig[...]
    for o in range(8):
        base = eig_row + tab[ROWTAB + 8 * o : ROWTAB + 8 * o + 8, NZ : 2 * NZ]
        for p in range(2):
            for j in range(H):
                recip[p, j, 8 * o : 8 * o + 8, :] = 1.0 / (base + float(LAM_T[2 * j + p]))
    copies[2].wait()
    copies[3].wait()
    mass_col = jnp.broadcast_to(mass[...], (NZ, NZ)).T
    w = split(mass_col * modes[...])
    w = block_diag2(w[0]), block_diag2(w[1])
    kyp = two(ky)
    for g in range(8):
        if g == 0:
            copies[4].wait()
            copies[5].wait()
        if g == 4:
            copies[6].wait()
        near = src[4 * g : 4 * g + 4].reshape(4 * T, NZ)
        far = jnp.concatenate([src[63 - 4 * g - i] for i in range(4)], axis=0)
        folded = split(jnp.concatenate([near + far, near - far], axis=1))
        modal = split(dot3(folded, w))
        ybuf[4 * g : 4 * g + 4] = dot3(kyp, modal).reshape(4, T, 2 * NZ)
    across = [[None] * 8, [None] * 8]
    along = []
    for p in range(2):
        kxp = two(kx, p)
        acc_y = [None] * H
        for q in range(4):
            parts = [
                ybuf[:, 8 * o : 8 * o + 8, p * NZ : (p + 1) * NZ].reshape(8 * H, NZ)
                for o in (2 * q, 2 * q + 1)
            ]
            spec = dot3(kxp, split(jnp.concatenate(parts, axis=1)))
            for i in range(2):
                o = 2 * q + i
                block = spec[:, i * NZ : (i + 1) * NZ]
                coef[p, :, 8 * o : 8 * o + 8, :] = block.reshape(H, 8, NZ)
                edge_b = tab[ROWTAB + 8 * o : ROWTAB + 8 * o + 8, 0:NZ]
                acc_x = None
                for j in range(H):
                    v = block[8 * j : 8 * j + 8] * recip[p, j, 8 * o : 8 * o + 8, :]
                    vx = v * float(EDGE[2 * j + p])
                    vy = v * edge_b
                    acc_x = vx if acc_x is None else acc_x + vx
                    acc_y[j] = vy if acc_y[j] is None else acc_y[j] + vy
                across[p][o] = acc_x
        along.append(jnp.concatenate(acc_y, axis=0))
    copies[7].wait()
    even = jnp.concatenate(across[0], axis=0)
    odd = jnp.concatenate(across[1], axis=0)
    sums = split(jnp.concatenate(along, axis=1))
    sel = wide[YSEL : YSEL + T, :]
    ends = dot(sel, sums[0]) + dot(sel, sums[1])
    first = jnp.concatenate([ends[:H, :NZ], ends[:H, NZ:]], axis=0)
    last = jnp.concatenate([ends[H:, :NZ], ends[H:, NZ:]], axis=0)
    xs = jnp.concatenate([even + odd, even - odd], axis=0)
    ys = jnp.concatenate([first, last], axis=0)
    edges[pl.ds(0, NZ, stride=2), :] = xs.T
    edges[pl.ds(1, NZ, stride=2), :] = ys.T


def turned(m):
    return jnp.concatenate([m[PY * (PX - 1 - i) : PY * (PX - i)] for i in range(PX)], axis=0)


def swap(m):
    return pltpu.roll(m, T, 1)


def interface_kernel(got, eig, tab, wide, out, xbuf):
    block = lambda at: wide[at : at + 256, :]
    cyl = [(block(CYL + 512 * i), block(CYL + 512 * i + 256)) for i in range(2)]
    mode = lax.axis_index("px") * PY + lax.axis_index("py")
    mu = jnp.sum(jnp.where(lanes((1, NZ), 1) == mode, eig[...], 0.0), axis=1, keepdims=True)
    lane = lanes((NZ, NZ), 1)
    low = lane < T
    low32 = low[: 2 * PX]
    low16 = low[:PX]
    low64 = low[:T]
    sign_b = jnp.where(lanes((2 * PX, NZ), 1) % 2 == 0, 1.0, -1.0)
    sign_a = jnp.where(lanes((T, NZ), 1) % T < H, 1.0, -1.0)
    gx = got[pl.ds(0, NZ, stride=2), :]
    gy = got[pl.ds(1, NZ, stride=2), :]

    mirror = swap(turned(gx))
    xbuf[...] = jnp.where(low, gx + mirror, swap(gx - mirror))
    tiles = []
    for q in range(4):
        rows = []
        for i in range(2):
            d = xbuf[pl.ds(2 * q + i, PX, stride=PY), :]
            other = swap(d)
            rows.append(jnp.concatenate([d, other] if i == 0 else [other, d], axis=0))
        tiles.append(jnp.where(low32, rows[0], rows[1]))
    flipped = [sign_b * swap(tiles[3 - q]) for q in range(2)]
    line_e = jnp.concatenate([tiles[q] + flipped[q] for q in range(2)], axis=1)
    line_o = jnp.concatenate([tiles[q] - flipped[q] for q in range(2)], axis=1)
    t1 = jnp.concatenate(
        [dot3(split(line_e), cyl[0]), dot3(split(line_o), cyl[1])], axis=1
    )
    t1h, t1l = split(t1)

    back = turned(gy)[:T]
    part_e = gy[:T] + sign_a * back
    part_o = gy[:T] - sign_a * back
    ends = jnp.concatenate(
        [jnp.where(low64, part_e, swap(part_o)), jnp.where(low64, swap(part_e), part_o)], axis=0
    ).T
    by_h, by_l = [
        jnp.concatenate([wide[at : at + NZ, :], wide[at + NZ : at + 2 * NZ, :]], axis=1)
        for at in (BYS, BYS + 256)
    ]
    by_lh = jnp.concatenate([by_l, by_h], axis=0)
    lam_y = jnp.concatenate([tab[LAM_Y : LAM_Y + 1, :], tab[LAM_Y + 1 : LAM_Y + 2, :]], axis=1)
    shift = lam_y + mu
    back_x, back_y = [], []
    for p in range(2):
        e = split(ends[T * p : T * p + T])
        eh, el = block_diag2(e[0]), block_diag2(e[1])
        ehh = jnp.concatenate([eh, eh], axis=0)
        th, tl = t1h[PX * p : PX * p + PX], t1l[PX * p : PX * p + PX]
        pad = jnp.zeros((NZ - 3 * PX, NY), BF16)
        weights = jnp.concatenate([by_h, th, th, tl, pad], axis=0)
        sum_x = sum_y = None
        for c in range(2):
            m = block(M12 + 512 * p + 256 * c)
            zz = dot(m, ehh) + dot(m[:, :NZ], el)
            zz = (zz.reshape(16, 16, 256) * tab[TZ + 16 * p : TZ + 16 * p + 16, :][None]).reshape(256, 256)
            zh, zl = split(zz[:, :NZ] + zz[:, NZ:])
            bk = wide[BKX + 256 * p : BKX + 256 * p + 256, NZ * c : NZ * c + NZ]
            spec = dot(jnp.concatenate([zh, bk], axis=1), weights)
            spec += dot(jnp.concatenate([zh, zl], axis=1), by_lh)
            lams = bk[:, 48:51].astype(F32)
            lam = (lams[:, 2:3] + lams[:, 1:2]) + lams[:, 0:1]
            u = split(spec / (shift + lam))
            at = [BKXT + 64 * p + 32 * h + 16 * c for h in range(2)]
            bx = dot3((wide[at[0] : at[0] + 16, :], wide[at[1] : at[1] + 16, :]), u)
            r = dot3((by_h, by_l), u, NT)
            turns = [
                jnp.concatenate([tab[TR + NZ * p : TR + NZ * p + NZ, NZ * i : NZ * i + NZ]] * 2, axis=1)
                for i in range(2)
            ]
            rh, rl = split(jnp.concatenate([r * turns[0], r * turns[1]], axis=0))
            both = dot(rh, m)
            by = both[:, :NZ] + both[:, NZ:] + dot(rl, m[:, :NZ])
            sum_x = bx if c == 0 else sum_x + bx
            sum_y = by if c == 0 else sum_y + by
        back_x.append(sum_x)
        back_y.append(sum_y[:NZ] + swap(sum_y[NZ:]))

    bx = jnp.concatenate(back_x, axis=0)
    we = dot3(split(bx[:, : NY // 2]), cyl[0], NT)
    wo = dot3(split(bx[:, NY // 2 :]), cyl[1], NT)
    near = we + wo
    far = we - wo
    for q in range(4):
        if q < 2:
            t = near[:, q * NZ : (q + 1) * NZ]
        else:
            t = swap(sign_b * far[:, (3 - q) * NZ : (4 - q) * NZ])
        s0 = t[:PX] + t[PX:]
        s1 = t[:PX] - t[PX:]
        xbuf[pl.ds(2 * q, PX, stride=PY), :] = jnp.where(low16, s0, swap(s1))
        xbuf[pl.ds(2 * q + 1, PX, stride=PY), :] = jnp.where(low16, swap(s0), s1)
    w = xbuf[...]
    other = swap(gx)
    own = jnp.where(
        low,
        jnp.concatenate([gx[:PY], other[:-PY]], axis=0),
        jnp.concatenate([other[PY:], gx[-PY:]], axis=0),
    )
    out[pl.ds(0, NZ, stride=2), :] = jnp.where(low, w, turned(w)) + own

    near = back_y[0] + back_y[1]
    far = back_y[0] - back_y[1]
    near = jnp.where(low64, near[:T], swap(near[T:]))
    far = sign_a * jnp.where(low64, far[:T], swap(far[T:]))
    w = jnp.concatenate([near, turned(jnp.concatenate([far, far], axis=0))[:T]], axis=0)
    row = lanes((NZ, NZ), 0) % PY
    other = swap(gy)
    own = jnp.where(
        low,
        jnp.where(row == 0, gy, pltpu.roll(other, 1, 0)),
        jnp.where(row == PY - 1, gy, pltpu.roll(other, NZ - 1, 0)),
    )
    out[pl.ds(1, NZ, stride=2), :] = w + own


def backward_kernel(coef, recip, got, modes, ky, kxt, tab, dest, ybuf, qbuf, obuf, sems):
    qbuf[0:NZ] = got[pl.ds(0, NZ, stride=2), :].T
    qbuf[NZ : 2 * NZ] = got[pl.ds(1, NZ, stride=2), :].T
    sign = jnp.where(lanes((8, NZ), 0) % 2 == 0, 1.0, -1.0)
    w = split(modes[...].T)
    w = block_diag2(w[0]), block_diag2(w[1])
    for p in range(2):
        kxp = two(kxt, p)
        ends = []
        for j in range(H):
            at = NZ + p * H + j
            ends.append(qbuf[at : at + 1] + sign * qbuf[at + T : at + T + 1])
        for q in range(4):
            parts = []
            for o in (2 * q, 2 * q + 1):
                near = qbuf[8 * o : 8 * o + 8]
                far = qbuf[T + 8 * o : T + 8 * o + 8]
                line = near + far if p == 0 else near - far
                edge_b = tab[ROWTAB + 8 * o : ROWTAB + 8 * o + 8, 0:NZ]
                blocks = []
                for j in range(H):
                    edge = line * float(EDGE[2 * j + p]) + ends[j] * edge_b
                    r = coef[p, j, 8 * o : 8 * o + 8, :] + edge
                    blocks.append(r * recip[p, j, 8 * o : 8 * o + 8, :])
                parts.append(jnp.concatenate(blocks, axis=0))
            back = dot3(kxp, split(jnp.concatenate(parts, axis=1)))
            for i in range(2):
                o = 2 * q + i
                ybuf[:, 8 * o : 8 * o + 8, p * NZ : (p + 1) * NZ] = back[
                    :, i * NZ : (i + 1) * NZ
                ].reshape(H, 8, NZ)
    kyp = two(ky)
    copies = []
    for g in range(8):
        block = split(ybuf[4 * g : 4 * g + 4].reshape(4 * T, 2 * NZ))
        modal = split(dot3(kyp, block))
        res = dot3(modal, w)
        near = res[:, :NZ]
        far = res[:, NZ:]
        obuf[4 * g : 4 * g + 4] = (near + far).reshape(4, T, NZ)
        other = near - far
        for i in range(4):
            obuf[63 - 4 * g - i] = other[T * i : T * i + T]
        for lo, hi in SENDS.get(g, ()):
            i = len(copies)
            copies.append(pltpu.make_async_copy(obuf.at[lo:hi], dest.at[lo:hi], sems.at[i]))
            copies[i].start()
    for copy in copies:
        copy.wait()


SENDS = {3: ((0, 16), (48, 64)), 5: ((16, 24), (40, 48)), 7: ((24, 40),)}
VMEM = pl.BlockSpec(memory_space=pltpu.VMEM)
HBM = pl.BlockSpec(memory_space=pltpu.HBM)
INTERPRET = False


def like(array):
    return jax.ShapeDtypeStruct(array.shape, array.dtype)


def exchange(value):
    value = value.reshape(NZ, 1, 2 * NZ)
    value = lax.all_to_all(value, AXES, split_axis=0, concat_axis=0, tiled=True)
    return value.reshape(2 * NZ, NZ)


def shards(source, layer_mass, modes, mode_eigen):
    tab, wide = solve_tables()
    params = pltpu.CompilerParams(vmem_limit_bytes=40 * 1024 * 1024)
    eig = mode_eigen[None]
    mass = layer_mass[None]
    edge_shape = jax.ShapeDtypeStruct((2 * NZ, NZ), F32)
    field = jax.ShapeDtypeStruct((2, H, T, NZ), F32)
    kron = (2, 8 * H, 8 * H)
    operands = [
        pltpu.with_memory_space_constraint(jnp.asarray(v), pltpu.HBM)
        for v in (source, mass, modes, eig, tab, wide)
    ]
    coef, recip, edges, ky, kxt, modes, eig, tab, wide = pl.pallas_call(
        forward_kernel,
        out_shape=(
            field,
            field,
            edge_shape,
            jax.ShapeDtypeStruct(kron, BF16),
            jax.ShapeDtypeStruct((2, *kron), BF16),
            like(modes),
            like(eig),
            like(tab),
            like(wide),
        ),
        in_specs=[HBM] * 6,
        out_specs=[VMEM] * 9,
        scratch_shapes=[
            pltpu.VMEM((T, T, NZ), F32),
            pltpu.VMEM((1, NZ), F32),
            pltpu.VMEM((2, *kron), BF16),
            pltpu.VMEM((H, T, 2 * NZ), F32),
            pltpu.SemaphoreType.DMA((8,)),
        ],
        compiler_params=params,
        interpret=INTERPRET,
        name="forward",
    )(*operands)
    values = pl.pallas_call(
        interface_kernel,
        out_shape=edge_shape,
        in_specs=[VMEM] * 4,
        out_specs=VMEM,
        scratch_shapes=[pltpu.VMEM((NZ, NZ), F32)],
        compiler_params=params,
        interpret=INTERPRET,
        name="interface",
    )(exchange(edges), eig, tab, wide)
    return pl.pallas_call(
        backward_kernel,
        out_shape=jax.ShapeDtypeStruct((T, T, NZ), F32),
        in_specs=[VMEM] * 7,
        out_specs=HBM,
        scratch_shapes=[
            pltpu.VMEM((H, T, 2 * NZ), F32),
            pltpu.VMEM((2 * NZ, NZ), F32),
            pltpu.VMEM((T, T, NZ), F32),
            pltpu.SemaphoreType.DMA((5,)),
        ],
        compiler_params=params,
        interpret=INTERPRET,
        name="backward",
    )(coef, recip, exchange(values), modes, ky, kxt, tab)


def solution(mesh):
    placed = (P("px", "py", None), P(), P(), P())
    return jax.shard_map(
        shards, mesh=mesh, in_specs=placed, out_specs=P("px", "py", None), check_vma=False
    )
```

```python
import jax
import jax.numpy as jnp
import numpy as np
from jax import lax
from jax.experimental import pallas as pl
from jax.experimental.pallas import tpu as pltpu
from jax.sharding import PartitionSpec as P

NX, NY, NZ = 1024, 512, 128
PX, PY = 16, 8
T = 64
H = T // 2
F32 = jnp.float32
BF16 = jnp.bfloat16
AXES = ("px", "py")


def np_split(table):
    table = np.asarray(table, np.float64)
    high = table.astype(np.float32).astype(jnp.bfloat16)
    low = (table - high.astype(np.float64)).astype(np.float32).astype(jnp.bfloat16)
    return high, low


def pair(table):
    return np.stack(np_split(table))


def sine_table():
    a = np.arange(1, T + 1)
    return np.sqrt(2.0 / (T + 1)) * np.sin(np.pi * np.outer(a, a) / (T + 1))


SINE = sine_table()
EDGE = SINE[:, 0]
LAM_T = 2.0 - 2.0 * np.cos(np.pi * np.arange(1, T + 1) / (T + 1))
ORDER_A = np.concatenate([np.arange(0, T, 2), np.arange(1, T, 2)])


def norm_row(length):
    return np.where(np.arange(length) == 0, np.sqrt(1.0 / length), np.sqrt(2.0 / length))


def tile_tables():
    rows = [SINE[p::2, :H] for p in range(2)] + [SINE[p::2, :H].T for p in range(2)]
    spread = np.concatenate([np.repeat(r, 8, axis=1) for r in rows])
    small = np.concatenate([spread, np.tile(SINE, (1, 4))]).astype(np.float32)
    edge_b = np.broadcast_to(EDGE[:, None], (T, NZ))
    lam_b = np.broadcast_to(LAM_T[:, None], (T, NZ))
    rowtab = np.concatenate([edge_b, lam_b], axis=1).astype(np.float32)
    signs = np.stack([np.ones(8), (-1.0) ** np.arange(8)])
    ysel = np.concatenate([np.kron(np.eye(H), signs[s : s + 1]) for s in range(2)])
    return small, rowtab, ysel.astype(jnp.bfloat16)


def solve_tables():
    al, be = np.arange(NX), np.arange(NY)
    sx, sy = norm_row(NX), norm_row(NY)
    by_parity = lambda n: np.concatenate([np.arange(0, n, 2), np.arange(1, n, 2)])
    al, be = by_parity(NX), by_parity(NY)
    sx, sy = sx[al], sy[be]
    local = np.arange(T) + 0.5
    lines_x = T * np.arange(PX) - 0.5
    lines_y = np.stack([T * np.arange(PY) - 0.5, T * np.arange(PY) + T + 0.5])
    bkx = sx[:, None] * np.cos(np.pi * al[:, None] * lines_x[None] / NX)
    bky = sy[:, None] * np.cos(np.pi * be[:, None] * lines_y.reshape(1, -1) / NY)
    bky = bky.reshape(NY, 2, 1, PY)
    bys = np.broadcast_to(bky, (NY, 2, PX // 2, PY)).reshape(NY, PX * PY).T
    place = np.arange(NY // 2) + 0.5
    cy = sy[:, None] * np.cos(np.pi * be[:, None] * place[None] / NY)
    cyl = np.einsum("bpy,cy->pcb", cy.reshape(NY, PY // 2, T), SINE).reshape(NY // 2, NY)
    cyl = np.stack([pair(cyl[:, : NY // 2]), pair(cyl[:, NY // 2 :])])
    phase = np.pi * al[:, None] * local[None] / NX
    m1 = (sx[:, None] * np.cos(phase)) @ SINE[:, ORDER_A]
    m2 = (sx[:, None] * np.sin(phase)) @ SINE[:, ORDER_A]
    m12 = np.concatenate(np_split(np.concatenate([m1, m2], axis=1)), axis=1)
    lam_x = 2.0 - 2.0 * np.cos(np.pi * al / NX)
    lam_h, lam_l = np_split(lam_x)
    rest = lam_x - lam_h.astype(np.float64) - lam_l.astype(np.float64)
    bkx_h, bkx_l = np_split(bkx)
    lams = np.stack([lam_h, lam_l, np_split(rest)[0]], axis=1)
    bkx_all = np.zeros((NX, 128), jnp.bfloat16)
    for i, part in enumerate((bkx_h, bkx_l, bkx_h, lams)):
        bkx_all[:, 16 * i : 16 * i + part.shape[1]] = part
    bkxt = np.stack([pair(bkx[512 * p : 512 * p + 512].T) for p in range(2)])
    px = np.arange(PX // 2)
    tz, tr = [], []
    for p in range(2):
        turn = np.pi * (2 * np.arange(16) + p)[:, None] * px[None] / PX
        wide = [np.tile(np.repeat(t, PY, axis=1), (1, 2)) for t in (np.cos(turn), -np.sin(turn))]
        tz.append(np.concatenate(wide, axis=1))
        tr += [np.tile(t.T, (1, 8)) for t in wide]
    tz = np.concatenate(tz).astype(np.float32)
    tr = np.stack(tr).astype(np.float32)
    lam_y = (2.0 - 2.0 * np.cos(np.pi * be / NY)).astype(np.float32)[None]
    bys = pair(bys)
    bys = np.concatenate([bys[:, :, :256], bys[:, :, 256:]], axis=1)
    bkx_all = bkx_all.reshape(2, 2, 256, 128)
    bkx_all = np.concatenate([bkx_all[:, 0], bkx_all[:, 1]], axis=2)
    bkxt = bkxt.reshape(2, 2, 16, 2, 256).transpose(0, 1, 3, 2, 4)
    tr = np.stack([np.concatenate([tr[2 * p], tr[2 * p + 1]], axis=1) for p in range(2)])
    small, rowtab, ysel = tile_tables()
    lam_y = np.concatenate([lam_y.reshape(2, 256), np.zeros((6, 256), np.float32)])
    flat = lambda parts: np.concatenate([t.reshape(-1, 256) for t in parts])
    return flat([small, rowtab, tz, tr, lam_y]), flat([cyl, m12, bkx_all, bys, bkxt, ysel])


SMALL, ROWTAB, TZ, TR, LAM_Y = 0, 192, 256, 288, 544
CYL, M12, BKX, BYS, BKXT, YSEL = 0, 1024, 2048, 2560, 3072, 3200


def split(value):
    high = value.astype(BF16)
    return high, (value - high.astype(F32)).astype(BF16)


PLAIN = (((1,), (0,)), ((), ()))
NT = (((1,), (1,)), ((), ()))


def dot(a, b, dims=PLAIN):
    return lax.dot_general(a, b, dims, preferred_element_type=F32)


def dot3(a, b, dims=PLAIN):
    return dot(a[0], b[0], dims) + dot(a[0], b[1], dims) + dot(a[1], b[0], dims)


def block_diag2(w):
    zero = jnp.zeros_like(w)
    top = jnp.concatenate([w, zero], axis=1)
    bottom = jnp.concatenate([zero, w], axis=1)
    return jnp.concatenate([top, bottom], axis=0)


def two(ref, *index):
    return ref[(*index, 0)], ref[(*index, 1)]


def lanes(shape, axis):
    return lax.broadcasted_iota(jnp.int32, shape, axis)


def forward_kernel(
    src_in, mass_in, modes_in, eig_in, tab_in, wide_in,
    coef, recip, edges, ky, kxt, modes, eig, tab, wide,
    src, mass, kx, ybuf, sems,
):
    jobs = [(tab_in, tab), (eig_in, eig), (mass_in, mass), (modes_in, modes)]
    for lo, hi in ((0, 16), (48, 64), (16, 48)):
        jobs.append((src_in.at[lo:hi], src.at[lo:hi]))
    jobs.append((wide_in, wide))
    copies = [pltpu.make_async_copy(a, b, sems.at[i]) for i, (a, b) in enumerate(jobs)]
    for copy in copies:
        copy.start()
    copies[0].wait()
    row_block = lanes((T, 4 * T), 1) // T
    for i in range(4):
        part = split(jnp.where(row_block == i, tab[4 * H : 4 * H + T, :], 0.0))
        for h in range(2):
            ky[h, T * i : T * i + T, :] = part[h]
    diagonal = lanes((8, 8 * H), 1) % 8 == lanes((8, 8 * H), 0)
    for t in range(4):
        spread = [jnp.where(diagonal, tab[H * t + j : H * t + j + 1, :], 0.0) for j in range(H)]
        part = split(jnp.concatenate(spread, axis=0))
        for h in range(2):
            if t < 2:
                kx[t, h] = part[h]
            else:
                kxt[t - 2, h] = part[h]
    copies[1].wait()
    eig_row = eig[...]
    for o in range(8):
        base = eig_row + tab[ROWTAB + 8 * o : ROWTAB + 8 * o + 8, NZ : 2 * NZ]
        for p in range(2):
            for j in range(H):
                recip[p, j, 8 * o : 8 * o + 8, :] = 1.0 / (base + float(LAM_T[2 * j + p]))
    copies[2].wait()
    copies[3].wait()
    mass_col = jnp.broadcast_to(mass[...], (NZ, NZ)).T
    w = split(mass_col * modes[...])
    w = block_diag2(w[0]), block_diag2(w[1])
    kyp = two(ky)
    for g in range(8):
        if g == 0:
            copies[4].wait()
            copies[5].wait()
        if g == 4:
            copies[6].wait()
        near = src[4 * g : 4 * g + 4].reshape(4 * T, NZ)
        far = jnp.concatenate([src[63 - 4 * g - i] for i in range(4)], axis=0)
        folded = split(jnp.concatenate([near + far, near - far], axis=1))
        modal = split(dot3(folded, w))
        ybuf[4 * g : 4 * g + 4] = dot3(kyp, modal).reshape(4, T, 2 * NZ)
    across = [[None] * 8, [None] * 8]
    along = []
    for p in range(2):
        kxp = two(kx, p)
        acc_y = [None] * H
        for q in range(4):
            parts = [
                ybuf[:, 8 * o : 8 * o + 8, p * NZ : (p + 1) * NZ].reshape(8 * H, NZ)
                for o in (2 * q, 2 * q + 1)
            ]
            spec = dot3(kxp, split(jnp.concatenate(parts, axis=1)))
            for i in range(2):
                o = 2 * q + i
                block = spec[:, i * NZ : (i + 1) * NZ]
                coef[p, :, 8 * o : 8 * o + 8, :] = block.reshape(H, 8, NZ)
                edge_b = tab[ROWTAB + 8 * o : ROWTAB + 8 * o + 8, 0:NZ]
                acc_x = None
                for j in range(H):
                    v = block[8 * j : 8 * j + 8] * recip[p, j, 8 * o : 8 * o + 8, :]
                    vx = v * float(EDGE[2 * j + p])
                    vy = v * edge_b
                    acc_x = vx if acc_x is None else acc_x + vx
                    acc_y[j] = vy if acc_y[j] is None else acc_y[j] + vy
                across[p][o] = acc_x
        along.append(jnp.concatenate(acc_y, axis=0))
    copies[7].wait()
    even = jnp.concatenate(across[0], axis=0)
    odd = jnp.concatenate(across[1], axis=0)
    sums = split(jnp.concatenate(along, axis=1))
    sel = wide[YSEL : YSEL + T, :]
    ends = dot(sel, sums[0]) + dot(sel, sums[1])
    first = jnp.concatenate([ends[:H, :NZ], ends[:H, NZ:]], axis=0)
    last = jnp.concatenate([ends[H:, :NZ], ends[H:, NZ:]], axis=0)
    xs = jnp.concatenate([even + odd, even - odd], axis=0)
    ys = jnp.concatenate([first, last], axis=0)
    edges[pl.ds(0, NZ, stride=2), :] = xs.T
    edges[pl.ds(1, NZ, stride=2), :] = ys.T


def turned(m):
    return jnp.concatenate([m[PY * (PX - 1 - i) : PY * (PX - i)] for i in range(PX)], axis=0)


def swap(m):
    return pltpu.roll(m, T, 1)


def interface_kernel(got, eig, tab, wide, out, xbuf):
    block = lambda at: wide[at : at + 256, :]
    cyl = [(block(CYL + 512 * i), block(CYL + 512 * i + 256)) for i in range(2)]
    mode = lax.axis_index("px") * PY + lax.axis_index("py")
    mu = jnp.sum(jnp.where(lanes((1, NZ), 1) == mode, eig[...], 0.0), axis=1, keepdims=True)
    lane = lanes((NZ, NZ), 1)
    low = lane < T
    low32 = low[: 2 * PX]
    low16 = low[:PX]
    low64 = low[:T]
    sign_b = jnp.where(lanes((2 * PX, NZ), 1) % 2 == 0, 1.0, -1.0)
    sign_a = jnp.where(lanes((T, NZ), 1) % T < H, 1.0, -1.0)
    gx = got[pl.ds(0, NZ, stride=2), :]
    gy = got[pl.ds(1, NZ, stride=2), :]

    mirror = swap(turned(gx))
    xbuf[...] = jnp.where(low, gx + mirror, swap(gx - mirror))
    tiles = []
    for q in range(4):
        rows = []
        for i in range(2):
            d = xbuf[pl.ds(2 * q + i, PX, stride=PY), :]
            other = swap(d)
            rows.append(jnp.concatenate([d, other] if i == 0 else [other, d], axis=0))
        tiles.append(jnp.where(low32, rows[0], rows[1]))
    flipped = [sign_b * swap(tiles[3 - q]) for q in range(2)]
    line_e = jnp.concatenate([tiles[q] + flipped[q] for q in range(2)], axis=1)
    line_o = jnp.concatenate([tiles[q] - flipped[q] for q in range(2)], axis=1)
    t1 = jnp.concatenate(
        [dot3(split(line_e), cyl[0]), dot3(split(line_o), cyl[1])], axis=1
    )
    t1h, t1l = split(t1)

    back = turned(gy)[:T]
    part_e = gy[:T] + sign_a * back
    part_o = gy[:T] - sign_a * back
    ends = jnp.concatenate(
        [jnp.where(low64, part_e, swap(part_o)), jnp.where(low64, swap(part_e), part_o)], axis=0
    ).T
    by_h, by_l = [
        jnp.concatenate([wide[at : at + NZ, :], wide[at + NZ : at + 2 * NZ, :]], axis=1)
        for at in (BYS, BYS + 256)
    ]
    by_lh = jnp.concatenate([by_l, by_h], axis=0)
    lam_y = jnp.concatenate([tab[LAM_Y : LAM_Y + 1, :], tab[LAM_Y + 1 : LAM_Y + 2, :]], axis=1)
    shift = lam_y + mu
    chunks = [(p, c) for p in range(2) for c in range(2)]
    m = [block(M12 + 512 * p + 256 * c) for p, c in chunks]
    starts = []
    weights = []
    pad = jnp.zeros((NZ - 3 * PX, NY), BF16)
    for p in range(2):
        e = split(ends[T * p : T * p + T])
        eh, el = block_diag2(e[0]), block_diag2(e[1])
        starts.append((jnp.concatenate([eh, eh], axis=0), el))
        th, tl = t1h[PX * p : PX * p + PX], t1l[PX * p : PX * p + PX]
        weights.append(jnp.concatenate([by_h, th, th, tl, pad], axis=0))
    zs = []
    for i, (p, c) in enumerate(chunks):
        zz = dot(m[i], starts[p][0]) + dot(m[i][:, :NZ], starts[p][1])
        turn = tab[TZ + 16 * p : TZ + 16 * p + 16, :][None]
        zz = (zz.reshape(16, 16, 256) * turn).reshape(256, 256)
        zs.append(split(zz[:, :NZ] + zz[:, NZ:]))
    us = []
    for i, (p, c) in enumerate(chunks):
        zh, zl = zs[i]
        bk = wide[BKX + 256 * p : BKX + 256 * p + 256, NZ * c : NZ * c + NZ]
        spec = dot(jnp.concatenate([zh, bk], axis=1), weights[p])
        spec += dot(jnp.concatenate([zh, zl], axis=1), by_lh)
        lams = bk[:, 48:51].astype(F32)
        lam = (lams[:, 2:3] + lams[:, 1:2]) + lams[:, 0:1]
        us.append(split(spec / (shift + lam)))
    bxs, rs = [], []
    for i, (p, c) in enumerate(chunks):
        r = dot3((by_h, by_l), us[i], NT)
        turns = [
            jnp.concatenate([tab[TR + NZ * p : TR + NZ * p + NZ, NZ * j : NZ * j + NZ]] * 2, axis=1)
            for j in range(2)
        ]
        rs.append(split(jnp.concatenate([r * turns[0], r * turns[1]], axis=0)))
        at = [BKXT + 64 * p + 32 * h + 16 * c for h in range(2)]
        bxs.append(dot3((wide[at[0] : at[0] + 16, :], wide[at[1] : at[1] + 16, :]), us[i]))
    bys = []
    for i in range(4):
        rh, rl = rs[i]
        both = dot(rh, m[i])
        bys.append(both[:, :NZ] + both[:, NZ:] + dot(rl, m[i][:, :NZ]))
    back_x = [bxs[0] + bxs[1], bxs[2] + bxs[3]]
    back_y = [bys[0] + bys[1], bys[2] + bys[3]]
    back_y = [y[:NZ] + swap(y[NZ:]) for y in back_y]

    bx = jnp.concatenate(back_x, axis=0)
    we = dot3(split(bx[:, : NY // 2]), cyl[0], NT)
    wo = dot3(split(bx[:, NY // 2 :]), cyl[1], NT)
    near = we + wo
    far = we - wo
    for q in range(4):
        if q < 2:
            t = near[:, q * NZ : (q + 1) * NZ]
        else:
            t = swap(sign_b * far[:, (3 - q) * NZ : (4 - q) * NZ])
        s0 = t[:PX] + t[PX:]
        s1 = t[:PX] - t[PX:]
        xbuf[pl.ds(2 * q, PX, stride=PY), :] = jnp.where(low16, s0, swap(s1))
        xbuf[pl.ds(2 * q + 1, PX, stride=PY), :] = jnp.where(low16, swap(s0), s1)
    w = xbuf[...]
    other = swap(gx)
    own = jnp.where(
        low,
        jnp.concatenate([gx[:PY], other[:-PY]], axis=0),
        jnp.concatenate([other[PY:], gx[-PY:]], axis=0),
    )
    out[pl.ds(0, NZ, stride=2), :] = jnp.where(low, w, turned(w)) + own

    near = back_y[0] + back_y[1]
    far = back_y[0] - back_y[1]
    near = jnp.where(low64, near[:T], swap(near[T:]))
    far = sign_a * jnp.where(low64, far[:T], swap(far[T:]))
    w = jnp.concatenate([near, turned(jnp.concatenate([far, far], axis=0))[:T]], axis=0)
    row = lanes((NZ, NZ), 0) % PY
    other = swap(gy)
    own = jnp.where(
        low,
        jnp.where(row == 0, gy, pltpu.roll(other, 1, 0)),
        jnp.where(row == PY - 1, gy, pltpu.roll(other, NZ - 1, 0)),
    )
    out[pl.ds(1, NZ, stride=2), :] = w + own


def backward_kernel(coef, recip, got, modes, ky, kxt, tab, dest, ybuf, qbuf, obuf, sems):
    qbuf[0:NZ] = got[pl.ds(0, NZ, stride=2), :].T
    qbuf[NZ : 2 * NZ] = got[pl.ds(1, NZ, stride=2), :].T
    sign = jnp.where(lanes((8, NZ), 0) % 2 == 0, 1.0, -1.0)
    w = split(modes[...].T)
    w = block_diag2(w[0]), block_diag2(w[1])
    for p in range(2):
        kxp = two(kxt, p)
        ends = []
        for j in range(H):
            at = NZ + p * H + j
            ends.append(qbuf[at : at + 1] + sign * qbuf[at + T : at + T + 1])
        for q in range(4):
            parts = []
            for o in (2 * q, 2 * q + 1):
                near = qbuf[8 * o : 8 * o + 8]
                far = qbuf[T + 8 * o : T + 8 * o + 8]
                line = near + far if p == 0 else near - far
                edge_b = tab[ROWTAB + 8 * o : ROWTAB + 8 * o + 8, 0:NZ]
                blocks = []
                for j in range(H):
                    edge = line * float(EDGE[2 * j + p]) + ends[j] * edge_b
                    r = coef[p, j, 8 * o : 8 * o + 8, :] + edge
                    blocks.append(r * recip[p, j, 8 * o : 8 * o + 8, :])
                parts.append(jnp.concatenate(blocks, axis=0))
            back = dot3(kxp, split(jnp.concatenate(parts, axis=1)))
            for i in range(2):
                o = 2 * q + i
                ybuf[:, 8 * o : 8 * o + 8, p * NZ : (p + 1) * NZ] = back[
                    :, i * NZ : (i + 1) * NZ
                ].reshape(H, 8, NZ)
    kyp = two(ky)
    copies = []
    for g in range(8):
        block = split(ybuf[4 * g : 4 * g + 4].reshape(4 * T, 2 * NZ))
        modal = split(dot3(kyp, block))
        res = dot3(modal, w)
        near = res[:, :NZ]
        far = res[:, NZ:]
        obuf[4 * g : 4 * g + 4] = (near + far).reshape(4, T, NZ)
        other = near - far
        for i in range(4):
            obuf[63 - 4 * g - i] = other[T * i : T * i + T]
        for lo, hi in SENDS.get(g, ()):
            i = len(copies)
            copies.append(pltpu.make_async_copy(obuf.at[lo:hi], dest.at[lo:hi], sems.at[i]))
            copies[i].start()
    for copy in copies:
        copy.wait()


SENDS = {3: ((0, 16), (48, 64)), 5: ((16, 24), (40, 48)), 7: ((24, 40),)}
VMEM = pl.BlockSpec(memory_space=pltpu.VMEM)
HBM = pl.BlockSpec(memory_space=pltpu.HBM)
INTERPRET = False


def like(array):
    return jax.ShapeDtypeStruct(array.shape, array.dtype)


def exchange(value):
    value = value.reshape(NZ, 1, 2 * NZ)
    value = lax.all_to_all(value, AXES, split_axis=0, concat_axis=0, tiled=True)
    return value.reshape(2 * NZ, NZ)


def shards(source, layer_mass, modes, mode_eigen):
    tab, wide = solve_tables()
    params = pltpu.CompilerParams(vmem_limit_bytes=40 * 1024 * 1024)
    eig = mode_eigen[None]
    mass = layer_mass[None]
    edge_shape = jax.ShapeDtypeStruct((2 * NZ, NZ), F32)
    field = jax.ShapeDtypeStruct((2, H, T, NZ), F32)
    kron = (2, 8 * H, 8 * H)
    operands = [
        pltpu.with_memory_space_constraint(jnp.asarray(v), pltpu.HBM)
        for v in (source, mass, modes, eig, tab, wide)
    ]
    coef, recip, edges, ky, kxt, modes, eig, tab, wide = pl.pallas_call(
        forward_kernel,
        out_shape=(
            field,
            field,
            edge_shape,
            jax.ShapeDtypeStruct(kron, BF16),
            jax.ShapeDtypeStruct((2, *kron), BF16),
            like(modes),
            like(eig),
            like(tab),
            like(wide),
        ),
        in_specs=[HBM] * 6,
        out_specs=[VMEM] * 9,
        scratch_shapes=[
            pltpu.VMEM((T, T, NZ), F32),
            pltpu.VMEM((1, NZ), F32),
            pltpu.VMEM((2, *kron), BF16),
            pltpu.VMEM((H, T, 2 * NZ), F32),
            pltpu.SemaphoreType.DMA((8,)),
        ],
        compiler_params=params,
        interpret=INTERPRET,
        name="forward",
    )(*operands)
    values = pl.pallas_call(
        interface_kernel,
        out_shape=edge_shape,
        in_specs=[VMEM] * 4,
        out_specs=VMEM,
        scratch_shapes=[pltpu.VMEM((NZ, NZ), F32)],
        compiler_params=params,
        interpret=INTERPRET,
        name="interface",
    )(exchange(edges), eig, tab, wide)
    return pl.pallas_call(
        backward_kernel,
        out_shape=jax.ShapeDtypeStruct((T, T, NZ), F32),
        in_specs=[VMEM] * 7,
        out_specs=HBM,
        scratch_shapes=[
            pltpu.VMEM((H, T, 2 * NZ), F32),
            pltpu.VMEM((2 * NZ, NZ), F32),
            pltpu.VMEM((T, T, NZ), F32),
            pltpu.SemaphoreType.DMA((5,)),
        ],
        compiler_params=params,
        interpret=INTERPRET,
        name="backward",
    )(coef, recip, exchange(values), modes, ky, kxt, tab)


def solution(mesh):
    placed = (P("px", "py", None), P(), P(), P())
    return jax.shard_map(
        shards, mesh=mesh, in_specs=placed, out_specs=P("px", "py", None), check_vma=False
    )
```

```python
import jax
import jax.numpy as jnp
import numpy as np
from jax import lax
from jax.experimental import pallas as pl
from jax.experimental.pallas import tpu as pltpu
from jax.sharding import PartitionSpec as P

NX, NY, NZ = 1024, 512, 128
PX, PY = 16, 8
T = 64
H = T // 2
F32 = jnp.float32
BF16 = jnp.bfloat16
AXES = ("px", "py")


def np_split(table):
    table = np.asarray(table, np.float64)
    high = table.astype(np.float32).astype(jnp.bfloat16)
    low = (table - high.astype(np.float64)).astype(np.float32).astype(jnp.bfloat16)
    return high, low


def pair(table):
    return np.stack(np_split(table))


def sine_table():
    a = np.arange(1, T + 1)
    return np.sqrt(2.0 / (T + 1)) * np.sin(np.pi * np.outer(a, a) / (T + 1))


SINE = sine_table()
EDGE = SINE[:, 0]
LAM_T = 2.0 - 2.0 * np.cos(np.pi * np.arange(1, T + 1) / (T + 1))
ORDER_A = np.concatenate([np.arange(0, T, 2), np.arange(1, T, 2)])


def norm_row(length):
    return np.where(np.arange(length) == 0, np.sqrt(1.0 / length), np.sqrt(2.0 / length))


def tile_tables():
    rows = [SINE[p::2, :H] for p in range(2)] + [SINE[p::2, :H].T for p in range(2)]
    spread = np.concatenate([np.repeat(r, 8, axis=1) for r in rows])
    small = np.concatenate([spread, np.tile(SINE, (1, 4))]).astype(np.float32)
    edge_b = np.broadcast_to(EDGE[:, None], (T, NZ))
    lam_b = np.broadcast_to(LAM_T[:, None], (T, NZ))
    rowtab = np.concatenate([edge_b, lam_b], axis=1).astype(np.float32)
    signs = np.stack([np.ones(8), (-1.0) ** np.arange(8)])
    ysel = np.concatenate([np.kron(np.eye(H), signs[s : s + 1]) for s in range(2)])
    return small, rowtab, ysel.astype(jnp.bfloat16)


def solve_tables():
    al, be = np.arange(NX), np.arange(NY)
    sx, sy = norm_row(NX), norm_row(NY)
    by_parity = lambda n: np.concatenate([np.arange(0, n, 2), np.arange(1, n, 2)])
    al, be = by_parity(NX), by_parity(NY)
    sx, sy = sx[al], sy[be]
    local = np.arange(T) + 0.5
    lines_x = T * np.arange(PX) - 0.5
    lines_y = np.stack([T * np.arange(PY) - 0.5, T * np.arange(PY) + T + 0.5])
    bkx = sx[:, None] * np.cos(np.pi * al[:, None] * lines_x[None] / NX)
    bky = sy[:, None] * np.cos(np.pi * be[:, None] * lines_y.reshape(1, -1) / NY)
    bky = bky.reshape(NY, 2, 1, PY)
    bys = np.broadcast_to(bky, (NY, 2, PX // 2, PY)).reshape(NY, PX * PY).T
    place = np.arange(NY // 2) + 0.5
    cy = sy[:, None] * np.cos(np.pi * be[:, None] * place[None] / NY)
    cyl = np.einsum("bpy,cy->pcb", cy.reshape(NY, PY // 2, T), SINE).reshape(NY // 2, NY)
    cyl = np.stack([pair(cyl[:, : NY // 2]), pair(cyl[:, NY // 2 :])])
    phase = np.pi * al[:, None] * local[None] / NX
    m1 = (sx[:, None] * np.cos(phase)) @ SINE[:, ORDER_A]
    m2 = (sx[:, None] * np.sin(phase)) @ SINE[:, ORDER_A]
    m12 = np.concatenate(np_split(np.concatenate([m1, m2], axis=1)), axis=1)
    lam_x = 2.0 - 2.0 * np.cos(np.pi * al / NX)
    lam_h, lam_l = np_split(lam_x)
    rest = lam_x - lam_h.astype(np.float64) - lam_l.astype(np.float64)
    bkx_h, bkx_l = np_split(bkx)
    lams = np.stack([lam_h, lam_l, np_split(rest)[0]], axis=1)
    bkx_all = np.zeros((NX, 128), jnp.bfloat16)
    for i, part in enumerate((bkx_h, bkx_l, bkx_h, lams)):
        bkx_all[:, 16 * i : 16 * i + part.shape[1]] = part
    bkxt = np.stack([pair(bkx[512 * p : 512 * p + 512].T) for p in range(2)])
    px = np.arange(PX // 2)
    tz, tr = [], []
    for p in range(2):
        turn = np.pi * (2 * np.arange(16) + p)[:, None] * px[None] / PX
        wide = [np.tile(np.repeat(t, PY, axis=1), (1, 2)) for t in (np.cos(turn), -np.sin(turn))]
        tz.append(np.concatenate(wide, axis=1))
        tr += [np.tile(t.T, (1, 8)) for t in wide]
    tz = np.concatenate(tz).astype(np.float32)
    tr = np.stack(tr).astype(np.float32)
    lam_y = (2.0 - 2.0 * np.cos(np.pi * be / NY)).astype(np.float32)[None]
    bys = pair(bys)
    bys = np.concatenate([bys[:, :, :256], bys[:, :, 256:]], axis=1)
    bkx_all = bkx_all.reshape(2, 2, 256, 128)
    bkx_all = np.concatenate([bkx_all[:, 0], bkx_all[:, 1]], axis=2)
    bkxt = bkxt.reshape(2, 2, 16, 2, 256).transpose(0, 1, 3, 2, 4)
    tr = np.stack([np.concatenate([tr[2 * p], tr[2 * p + 1]], axis=1) for p in range(2)])
    small, rowtab, ysel = tile_tables()
    lam_y = np.concatenate([lam_y.reshape(2, 256), np.zeros((6, 256), np.float32)])
    flat = lambda parts: np.concatenate([t.reshape(-1, 256) for t in parts])
    return flat([small, rowtab, tz, tr, lam_y]), flat([cyl, m12, bkx_all, bys, bkxt, ysel])


SMALL, ROWTAB, TZ, TR, LAM_Y = 0, 192, 256, 288, 544
CYL, M12, BKX, BYS, BKXT, YSEL = 0, 1024, 2048, 2560, 3072, 3200


def split(value):
    high = value.astype(BF16)
    return high, (value - high.astype(F32)).astype(BF16)


PLAIN = (((1,), (0,)), ((), ()))
NT = (((1,), (1,)), ((), ()))


def dot(a, b, dims=PLAIN):
    return lax.dot_general(a, b, dims, preferred_element_type=F32)


def dot3(a, b, dims=PLAIN):
    return dot(a[0], b[0], dims) + dot(a[0], b[1], dims) + dot(a[1], b[0], dims)


def halves(value, axis):
    size = value.shape[axis] // 2
    if axis == 0:
        return value[:size] + value[size:]
    return value[:, :size] + value[:, size:]


def vertical(rows, w):
    return halves(dot(jnp.concatenate(split(rows), axis=1), w), 1)


def vertical_table(w):
    both = jnp.concatenate(split(w), axis=1)
    return jnp.concatenate([both, both], axis=0)


def along_y(table, block):
    both = jnp.concatenate([block[: 2 * T], block[2 * T :]], axis=1)
    return halves(dot(table, jnp.concatenate(split(both), axis=0)), 0)


def block_diag2(w):
    zero = jnp.zeros_like(w)
    top = jnp.concatenate([w, zero], axis=1)
    bottom = jnp.concatenate([zero, w], axis=1)
    return jnp.concatenate([top, bottom], axis=0)


def two(ref, *index):
    return ref[(*index, 0)], ref[(*index, 1)]


def lanes(shape, axis):
    return lax.broadcasted_iota(jnp.int32, shape, axis)


def forward_kernel(
    src_in, mass_in, modes_in, eig_in, tab_in, wide_in,
    coef, recip, edges, ky, kxt, modes, eig, tab, wide,
    src, mass, kx, ybuf, sems,
):
    jobs = [(tab_in.at[:TZ], tab.at[:TZ]), (eig_in, eig), (mass_in, mass), (modes_in, modes)]
    jobs += [(src_in, src), (wide_in, wide), (tab_in.at[TZ:], tab.at[TZ:])]
    copies = [pltpu.make_async_copy(a, b, sems.at[i]) for i, (a, b) in enumerate(jobs)]
    for copy in copies:
        copy.start()
    copies[0].wait()
    row_block = lanes((T, 4 * T), 1) // T % 2
    for i in range(2):
        part = split(jnp.where(row_block == i, tab[4 * H : 4 * H + T, :], 0.0))
        for h in range(2):
            ky[2 * T * h + T * i : 2 * T * h + T * i + T, :] = part[h]
    diagonal = lanes((8, 8 * H), 1) % 8 == lanes((8, 8 * H), 0)
    for t in range(4):
        spread = [jnp.where(diagonal, tab[H * t + j : H * t + j + 1, :], 0.0) for j in range(H)]
        part = split(jnp.concatenate(spread, axis=0))
        for h in range(2):
            if t < 2:
                kx[t, h] = part[h]
            else:
                kxt[t - 2, h] = part[h]
    copies[1].wait()
    eig_row = eig[...]
    for o in range(8):
        base = eig_row + tab[ROWTAB + 8 * o : ROWTAB + 8 * o + 8, NZ : 2 * NZ]
        for p in range(2):
            for j in range(H):
                recip[p, j, 8 * o : 8 * o + 8, :] = 1.0 / (base + float(LAM_T[2 * j + p]))
    copies[2].wait()
    copies[3].wait()
    mass_col = jnp.broadcast_to(mass[...], (NZ, NZ)).T
    w = vertical_table(mass_col * modes[...])
    copies[4].wait()
    mods = [[], []]
    for g in range(8):
        near = src[4 * g : 4 * g + 4].reshape(4 * T, NZ)
        far = jnp.concatenate([src[63 - 4 * g - i] for i in range(4)], axis=0)
        mods[0].append(vertical(near + far, w))
        mods[1].append(vertical(near - far, w))
    table = ky[...]
    for p in range(2):
        for g in range(8):
            res = along_y(table, mods[p][g])
            for i in range(2):
                part = res[:, i * NZ : i * NZ + NZ].reshape(2, T, NZ)
                ybuf[4 * g + 2 * i : 4 * g + 2 * i + 2, :, p * NZ : p * NZ + NZ] = part
    across = [[None] * 8, [None] * 8]
    along = []
    for p in range(2):
        kxp = two(kx, p)
        acc_y = [None] * H
        for q in range(4):
            parts = [
                ybuf[:, 8 * o : 8 * o + 8, p * NZ : (p + 1) * NZ].reshape(8 * H, NZ)
                for o in (2 * q, 2 * q + 1)
            ]
            spec = dot3(kxp, split(jnp.concatenate(parts, axis=1)))
            for i in range(2):
                o = 2 * q + i
                block = spec[:, i * NZ : (i + 1) * NZ]
                coef[p, :, 8 * o : 8 * o + 8, :] = block.reshape(H, 8, NZ)
                edge_b = tab[ROWTAB + 8 * o : ROWTAB + 8 * o + 8, 0:NZ]
                acc_x = None
                for j in range(H):
                    v = block[8 * j : 8 * j + 8] * recip[p, j, 8 * o : 8 * o + 8, :]
                    vx = v * float(EDGE[2 * j + p])
                    vy = v * edge_b
                    acc_x = vx if acc_x is None else acc_x + vx
                    acc_y[j] = vy if acc_y[j] is None else acc_y[j] + vy
                across[p][o] = acc_x
        along.append(jnp.concatenate(acc_y, axis=0))
    copies[5].wait()
    copies[6].wait()
    even = jnp.concatenate(across[0], axis=0)
    odd = jnp.concatenate(across[1], axis=0)
    sums = split(jnp.concatenate(along, axis=1))
    sel = wide[YSEL : YSEL + T, :]
    ends = dot(sel, sums[0]) + dot(sel, sums[1])
    first = jnp.concatenate([ends[:H, :NZ], ends[:H, NZ:]], axis=0)
    last = jnp.concatenate([ends[H:, :NZ], ends[H:, NZ:]], axis=0)
    xs = jnp.concatenate([even + odd, even - odd], axis=0)
    ys = jnp.concatenate([first, last], axis=0)
    edges[pl.ds(0, NZ, stride=2), :] = xs.T
    edges[pl.ds(1, NZ, stride=2), :] = ys.T


def turned(m):
    return jnp.concatenate([m[PY * (PX - 1 - i) : PY * (PX - i)] for i in range(PX)], axis=0)


def swap(m):
    return pltpu.roll(m, T, 1)


def interface_kernel(got, eig, tab, wide, out, xbuf):
    block = lambda at: wide[at : at + 256, :]
    cyl = [(block(CYL + 512 * i), block(CYL + 512 * i + 256)) for i in range(2)]
    mode = lax.axis_index("px") * PY + lax.axis_index("py")
    mu = jnp.sum(jnp.where(lanes((1, NZ), 1) == mode, eig[...], 0.0), axis=1, keepdims=True)
    lane = lanes((NZ, NZ), 1)
    low = lane < T
    low32 = low[: 2 * PX]
    low16 = low[:PX]
    low64 = low[:T]
    sign_b = jnp.where(lanes((2 * PX, NZ), 1) % 2 == 0, 1.0, -1.0)
    sign_a = jnp.where(lanes((T, NZ), 1) % T < H, 1.0, -1.0)
    gx = got[pl.ds(0, NZ, stride=2), :]
    gy = got[pl.ds(1, NZ, stride=2), :]

    mirror = swap(turned(gx))
    xbuf[...] = jnp.where(low, gx + mirror, swap(gx - mirror))
    tiles = []
    for q in range(4):
        rows = []
        for i in range(2):
            d = xbuf[pl.ds(2 * q + i, PX, stride=PY), :]
            other = swap(d)
            rows.append(jnp.concatenate([d, other] if i == 0 else [other, d], axis=0))
        tiles.append(jnp.where(low32, rows[0], rows[1]))
    flipped = [sign_b * swap(tiles[3 - q]) for q in range(2)]
    line_e = jnp.concatenate([tiles[q] + flipped[q] for q in range(2)], axis=1)
    line_o = jnp.concatenate([tiles[q] - flipped[q] for q in range(2)], axis=1)
    t1 = jnp.concatenate(
        [dot3(split(line_e), cyl[0]), dot3(split(line_o), cyl[1])], axis=1
    )
    t1h, t1l = split(t1)

    back = turned(gy)[:T]
    part_e = gy[:T] + sign_a * back
    part_o = gy[:T] - sign_a * back
    ends = jnp.concatenate(
        [jnp.where(low64, part_e, swap(part_o)), jnp.where(low64, swap(part_e), part_o)], axis=0
    ).T
    by_h, by_l = [
        jnp.concatenate([wide[at : at + NZ, :], wide[at + NZ : at + 2 * NZ, :]], axis=1)
        for at in (BYS, BYS + 256)
    ]
    by_lh = jnp.concatenate([by_l, by_h], axis=0)
    by_hl = jnp.concatenate([by_h, by_l], axis=0)
    lam_y = jnp.concatenate([tab[LAM_Y : LAM_Y + 1, :], tab[LAM_Y + 1 : LAM_Y + 2, :]], axis=1)
    shift = lam_y + mu
    chunks = [(p, c) for p in range(2) for c in range(2)]
    m = [block(M12 + 512 * p + 256 * c) for p, c in chunks]
    starts = []
    weights = []
    pad = jnp.zeros((NZ - 3 * PX, NY), BF16)
    for p in range(2):
        e = split(ends[T * p : T * p + T])
        eh, el = block_diag2(e[0]), block_diag2(e[1])
        starts.append((jnp.concatenate([eh, eh], axis=0), el))
        th, tl = t1h[PX * p : PX * p + PX], t1l[PX * p : PX * p + PX]
        weights.append(jnp.concatenate([by_h, th, th, tl, pad], axis=0))
    zs = []
    for i, (p, c) in enumerate(chunks):
        zz = dot(m[i], starts[p][0]) + dot(m[i][:, :NZ], starts[p][1])
        turn = tab[TZ + 16 * p : TZ + 16 * p + 16, :][None]
        zz = (zz.reshape(16, 16, 256) * turn).reshape(256, 256)
        zs.append(split(zz[:, :NZ] + zz[:, NZ:]))
    us, bxs, rs = [], [], []
    turns = [
        [
            jnp.concatenate([tab[TR + NZ * p : TR + NZ * p + NZ, NZ * j : NZ * j + NZ]] * 2, axis=1)
            for j in range(2)
        ]
        for p in range(2)
    ]
    for step in range(5):
        if step < 4:
            p, c = chunks[step]
            zh, zl = zs[step]
            bk = wide[BKX + 256 * p : BKX + 256 * p + 256, NZ * c : NZ * c + NZ]
            spec = dot(jnp.concatenate([zh, bk], axis=1), weights[p])
            spec += dot(jnp.concatenate([zh, zl], axis=1), by_lh)
            lams = bk[:, 48:51].astype(F32)
            lam = (lams[:, 2:3] + lams[:, 1:2]) + lams[:, 0:1]
            us.append(split(spec / (shift + lam)))
        if step > 0:
            p, c = chunks[step - 1]
            u = us[step - 1]
            r = halves(dot(by_hl, u[0], NT), 0) + dot(by_h, u[1], NT)
            rs.append(split(jnp.concatenate([r * turns[p][0], r * turns[p][1]], axis=0)))
            at = [BKXT + 64 * p + 32 * h + 16 * c for h in range(2)]
            lines = jnp.concatenate([wide[k : k + 16, :] for k in at], axis=0)
            bxs.append(halves(dot(lines, u[0]), 0) + dot(lines[:16], u[1]))
    bys = []
    for i in range(4):
        rh, rl = rs[i]
        both = dot(rh, m[i])
        bys.append(both[:, :NZ] + both[:, NZ:] + dot(rl, m[i][:, :NZ]))
    back_x = [bxs[0] + bxs[1], bxs[2] + bxs[3]]
    back_y = [bys[0] + bys[1], bys[2] + bys[3]]
    back_y = [y[:NZ] + swap(y[NZ:]) for y in back_y]

    bx = jnp.concatenate(back_x, axis=0)
    we = dot3(split(bx[:, : NY // 2]), cyl[0], NT)
    wo = dot3(split(bx[:, NY // 2 :]), cyl[1], NT)
    near = we + wo
    far = we - wo
    for q in range(4):
        if q < 2:
            t = near[:, q * NZ : (q + 1) * NZ]
        else:
            t = swap(sign_b * far[:, (3 - q) * NZ : (4 - q) * NZ])
        s0 = t[:PX] + t[PX:]
        s1 = t[:PX] - t[PX:]
        xbuf[pl.ds(2 * q, PX, stride=PY), :] = jnp.where(low16, s0, swap(s1))
        xbuf[pl.ds(2 * q + 1, PX, stride=PY), :] = jnp.where(low16, swap(s0), s1)
    w = xbuf[...]
    other = swap(gx)
    own = jnp.where(
        low,
        jnp.concatenate([gx[:PY], other[:-PY]], axis=0),
        jnp.concatenate([other[PY:], gx[-PY:]], axis=0),
    )
    out[pl.ds(0, NZ, stride=2), :] = jnp.where(low, w, turned(w)) + own

    near = back_y[0] + back_y[1]
    far = back_y[0] - back_y[1]
    near = jnp.where(low64, near[:T], swap(near[T:]))
    far = sign_a * jnp.where(low64, far[:T], swap(far[T:]))
    w = jnp.concatenate([near, turned(jnp.concatenate([far, far], axis=0))[:T]], axis=0)
    row = lanes((NZ, NZ), 0) % PY
    other = swap(gy)
    own = jnp.where(
        low,
        jnp.where(row == 0, gy, pltpu.roll(other, 1, 0)),
        jnp.where(row == PY - 1, gy, pltpu.roll(other, NZ - 1, 0)),
    )
    out[pl.ds(1, NZ, stride=2), :] = w + own


def backward_kernel(coef, recip, got, modes, ky, kxt, tab, dest, ybuf, qbuf, obuf, sems):
    qbuf[0:NZ] = got[pl.ds(0, NZ, stride=2), :].T
    qbuf[NZ : 2 * NZ] = got[pl.ds(1, NZ, stride=2), :].T
    sign = jnp.where(lanes((8, NZ), 0) % 2 == 0, 1.0, -1.0)
    w = vertical_table(modes[...].T)
    for p in range(2):
        kxp = two(kxt, p)
        ends = []
        for j in range(H):
            at = NZ + p * H + j
            ends.append(qbuf[at : at + 1] + sign * qbuf[at + T : at + T + 1])
        for q in range(4):
            parts = []
            for o in (2 * q, 2 * q + 1):
                near = qbuf[8 * o : 8 * o + 8]
                far = qbuf[T + 8 * o : T + 8 * o + 8]
                line = near + far if p == 0 else near - far
                edge_b = tab[ROWTAB + 8 * o : ROWTAB + 8 * o + 8, 0:NZ]
                blocks = []
                for j in range(H):
                    edge = line * float(EDGE[2 * j + p]) + ends[j] * edge_b
                    r = coef[p, j, 8 * o : 8 * o + 8, :] + edge
                    blocks.append(r * recip[p, j, 8 * o : 8 * o + 8, :])
                parts.append(jnp.concatenate(blocks, axis=0))
            back = dot3(kxp, split(jnp.concatenate(parts, axis=1)))
            for i in range(2):
                o = 2 * q + i
                ybuf[:, 8 * o : 8 * o + 8, p * NZ : (p + 1) * NZ] = back[
                    :, i * NZ : (i + 1) * NZ
                ].reshape(H, 8, NZ)
    table = ky[...]
    copies = []
    for g in range(8):
        outs = []
        for p in range(2):
            block = ybuf[4 * g : 4 * g + 4, :, p * NZ : p * NZ + NZ].reshape(4 * T, NZ)
            res = along_y(table, block)
            outs.append(vertical(jnp.concatenate([res[:, :NZ], res[:, NZ:]], axis=0), w))
        even, odd = outs
        obuf[4 * g : 4 * g + 4] = (even + odd).reshape(4, T, NZ)
        other = even - odd
        for i in range(4):
            obuf[63 - 4 * g - i] = other[T * i : T * i + T]
        for lo, hi in SENDS.get(g, ()):
            i = len(copies)
            copies.append(pltpu.make_async_copy(obuf.at[lo:hi], dest.at[lo:hi], sems.at[i]))
            copies[i].start()
    for copy in copies:
        copy.wait()


SENDS = {3: ((0, 16), (48, 64)), 5: ((16, 24), (40, 48)), 7: ((24, 40),)}
VMEM = pl.BlockSpec(memory_space=pltpu.VMEM)
HBM = pl.BlockSpec(memory_space=pltpu.HBM)
INTERPRET = False


def like(array):
    return jax.ShapeDtypeStruct(array.shape, array.dtype)


def exchange(value):
    value = value.reshape(NZ, 1, 2 * NZ)
    value = lax.all_to_all(value, AXES, split_axis=0, concat_axis=0, tiled=True)
    return value.reshape(2 * NZ, NZ)


def shards(source, layer_mass, modes, mode_eigen):
    tab, wide = solve_tables()
    params = pltpu.CompilerParams(vmem_limit_bytes=40 * 1024 * 1024)
    eig = mode_eigen[None]
    mass = layer_mass[None]
    edge_shape = jax.ShapeDtypeStruct((2 * NZ, NZ), F32)
    field = jax.ShapeDtypeStruct((2, H, T, NZ), F32)
    kron = (2, 8 * H, 8 * H)
    operands = [
        pltpu.with_memory_space_constraint(jnp.asarray(v), pltpu.HBM)
        for v in (source, mass, modes, eig, tab, wide)
    ]
    coef, recip, edges, ky, kxt, modes, eig, tab, wide = pl.pallas_call(
        forward_kernel,
        out_shape=(
            field,
            field,
            edge_shape,
            jax.ShapeDtypeStruct(kron[1:], BF16),
            jax.ShapeDtypeStruct((2, *kron), BF16),
            like(modes),
            like(eig),
            like(tab),
            like(wide),
        ),
        in_specs=[HBM] * 6,
        out_specs=[VMEM] * 9,
        scratch_shapes=[
            pltpu.VMEM((T, T, NZ), F32),
            pltpu.VMEM((1, NZ), F32),
            pltpu.VMEM((2, *kron), BF16),
            pltpu.VMEM((H, T, 2 * NZ), F32),
            pltpu.SemaphoreType.DMA((7,)),
        ],
        compiler_params=params,
        interpret=INTERPRET,
        name="forward",
    )(*operands)
    values = pl.pallas_call(
        interface_kernel,
        out_shape=edge_shape,
        in_specs=[VMEM] * 4,
        out_specs=VMEM,
        scratch_shapes=[pltpu.VMEM((NZ, NZ), F32)],
        compiler_params=params,
        interpret=INTERPRET,
        name="interface",
    )(exchange(edges), eig, tab, wide)
    return pl.pallas_call(
        backward_kernel,
        out_shape=jax.ShapeDtypeStruct((T, T, NZ), F32),
        in_specs=[VMEM] * 7,
        out_specs=HBM,
        scratch_shapes=[
            pltpu.VMEM((H, T, 2 * NZ), F32),
            pltpu.VMEM((2 * NZ, NZ), F32),
            pltpu.VMEM((T, T, NZ), F32),
            pltpu.SemaphoreType.DMA((5,)),
        ],
        compiler_params=params,
        interpret=INTERPRET,
        name="backward",
    )(coef, recip, exchange(values), modes, ky, kxt, tab)


def solution(mesh):
    placed = (P("px", "py", None), P(), P(), P())
    return jax.shard_map(
        shards, mesh=mesh, in_specs=placed, out_specs=P("px", "py", None), check_vma=False
    )
```

```python
import jax
import jax.numpy as jnp
import numpy as np
from jax import lax
from jax.experimental import pallas as pl
from jax.experimental.pallas import tpu as pltpu
from jax.sharding import PartitionSpec as P

NX, NY, NZ = 1024, 512, 128
PX, PY = 16, 8
T = 64
H = T // 2
F32 = jnp.float32
BF16 = jnp.bfloat16
AXES = ("px", "py")


def np_split(table):
    table = np.asarray(table, np.float64)
    high = table.astype(np.float32).astype(jnp.bfloat16)
    low = (table - high.astype(np.float64)).astype(np.float32).astype(jnp.bfloat16)
    return high, low


def pair(table):
    return np.stack(np_split(table))


def sine_table():
    a = np.arange(1, T + 1)
    return np.sqrt(2.0 / (T + 1)) * np.sin(np.pi * np.outer(a, a) / (T + 1))


SINE = sine_table()
EDGE = SINE[:, 0]
LAM_T = 2.0 - 2.0 * np.cos(np.pi * np.arange(1, T + 1) / (T + 1))
ORDER_A = np.concatenate([np.arange(0, T, 2), np.arange(1, T, 2)])


def norm_row(length):
    return np.where(np.arange(length) == 0, np.sqrt(1.0 / length), np.sqrt(2.0 / length))


def tile_tables():
    rows = [SINE[p::2, :H] for p in range(2)] + [SINE[p::2, :H].T for p in range(2)]
    spread = np.concatenate([np.repeat(r, 8, axis=1) for r in rows])
    small = np.concatenate([spread, np.tile(SINE, (1, 4))]).astype(np.float32)
    edge_b = np.broadcast_to(EDGE[:, None], (T, NZ))
    lam_b = np.broadcast_to(LAM_T[:, None], (T, NZ))
    rowtab = np.concatenate([edge_b, lam_b], axis=1).astype(np.float32)
    signs = np.stack([np.ones(8), (-1.0) ** np.arange(8)])
    ysel = np.concatenate([np.kron(np.eye(H), signs[s : s + 1]) for s in range(2)])
    return small, rowtab, ysel.astype(jnp.bfloat16)


def solve_tables():
    al, be = np.arange(NX), np.arange(NY)
    sx, sy = norm_row(NX), norm_row(NY)
    by_parity = lambda n: np.concatenate([np.arange(0, n, 2), np.arange(1, n, 2)])
    al, be = by_parity(NX), by_parity(NY)
    sx, sy = sx[al], sy[be]
    local = np.arange(T) + 0.5
    lines_x = T * np.arange(PX) - 0.5
    lines_y = np.stack([T * np.arange(PY) - 0.5, T * np.arange(PY) + T + 0.5])
    bkx = sx[:, None] * np.cos(np.pi * al[:, None] * lines_x[None] / NX)
    bky = sy[:, None] * np.cos(np.pi * be[:, None] * lines_y.reshape(1, -1) / NY)
    bky = bky.reshape(NY, 2, 1, PY)
    bys = np.broadcast_to(bky, (NY, 2, PX // 2, PY)).reshape(NY, PX * PY).T
    place = np.arange(NY // 2) + 0.5
    cy = sy[:, None] * np.cos(np.pi * be[:, None] * place[None] / NY)
    cyl = np.einsum("bpy,cy->pcb", cy.reshape(NY, PY // 2, T), SINE).reshape(NY // 2, NY)
    cyl = np.stack([pair(cyl[:, : NY // 2]), pair(cyl[:, NY // 2 :])])
    phase = np.pi * al[:, None] * local[None] / NX
    m1 = (sx[:, None] * np.cos(phase)) @ SINE[:, ORDER_A]
    m2 = (sx[:, None] * np.sin(phase)) @ SINE[:, ORDER_A]
    m12 = np.concatenate(np_split(np.concatenate([m1, m2], axis=1)), axis=1)
    lam_x = 2.0 - 2.0 * np.cos(np.pi * al / NX)
    bkx_h, bkx_l = np_split(bkx)
    bkx_all = np.zeros((NX, 128), jnp.bfloat16)
    for i, part in enumerate((bkx_h, bkx_l, bkx_h)):
        bkx_all[:, 16 * i : 16 * i + part.shape[1]] = part
    bkxt = np.stack([pair(bkx[512 * p : 512 * p + 512].T) for p in range(2)])
    px = np.arange(PX // 2)
    tz, tr = [], []
    for p in range(2):
        turn = np.pi * (2 * np.arange(16) + p)[:, None] * px[None] / PX
        wide = [np.tile(np.repeat(t, PY, axis=1), (1, 2)) for t in (np.cos(turn), -np.sin(turn))]
        tz.append(np.concatenate(wide, axis=1))
        tr += [np.tile(t.T, (1, 8)) for t in wide]
    tz = np.concatenate(tz).astype(np.float32)
    tr = np.stack(tr).astype(np.float32)
    lam_y = (2.0 - 2.0 * np.cos(np.pi * be / NY)).astype(np.float32)[None]
    bys = pair(bys)
    bys = np.concatenate([bys[:, :, :256], bys[:, :, 256:]], axis=1)
    bkx_all = bkx_all.reshape(2, 2, 256, 128)
    bkx_all = np.concatenate([bkx_all[:, 0], bkx_all[:, 1]], axis=2)
    bkxt = bkxt.reshape(2, 2, 16, 2, 256).transpose(0, 1, 3, 2, 4)
    tr = np.stack([np.concatenate([tr[2 * p], tr[2 * p + 1]], axis=1) for p in range(2)])
    small, rowtab, ysel = tile_tables()
    lams = [lam_y.reshape(2, 256), lam_x.astype(np.float32).reshape(4, 256)]
    lams = np.concatenate([*lams, np.zeros((2, 256), np.float32)])
    flat = lambda parts: np.concatenate([t.reshape(-1, 256) for t in parts])
    return flat([small, rowtab, lams, tz, tr]), flat([cyl, m12, bkx_all, bys, bkxt, ysel])


SMALL, ROWTAB, LAMS, TZ, TR = 0, 192, 256, 264, 296
CYL, M12, BKX, BYS, BKXT, YSEL = 0, 1024, 2048, 2560, 3072, 3200


def split(value):
    high = value.astype(BF16)
    return high, (value - high.astype(F32)).astype(BF16)


PLAIN = (((1,), (0,)), ((), ()))
NT = (((1,), (1,)), ((), ()))


def dot(a, b, dims=PLAIN):
    return lax.dot_general(a, b, dims, preferred_element_type=F32)


def dot3(a, b, dims=PLAIN):
    return dot(a[0], b[0], dims) + dot(a[0], b[1], dims) + dot(a[1], b[0], dims)


def halves(value, axis):
    size = value.shape[axis] // 2
    if axis == 0:
        return value[:size] + value[size:]
    return value[:, :size] + value[:, size:]


def vertical(rows, w):
    return halves(dot(jnp.concatenate(split(rows), axis=1), w), 1)


def vertical_table(w):
    both = jnp.concatenate(split(w), axis=1)
    return jnp.concatenate([both, both], axis=0)


def along_y(table, block):
    both = jnp.concatenate([block[: 2 * T], block[2 * T :]], axis=1)
    return halves(dot(table, jnp.concatenate(split(both), axis=0)), 0)


def block_diag2(w):
    zero = jnp.zeros_like(w)
    top = jnp.concatenate([w, zero], axis=1)
    bottom = jnp.concatenate([zero, w], axis=1)
    return jnp.concatenate([top, bottom], axis=0)


def two(ref, *index):
    return ref[(*index, 0)], ref[(*index, 1)]


def lanes(shape, axis):
    return lax.broadcasted_iota(jnp.int32, shape, axis)


def forward_kernel(
    src_in, mass_in, modes_in, eig_in, tab_in, wide_in,
    coef, recip, edges, ky, kxt, modes, tab, wide, scale,
    src, mass, eig, kx, ybuf, sems,
):
    jobs = [(tab_in.at[:TZ], tab.at[:TZ]), (eig_in, eig), (mass_in, mass), (modes_in, modes)]
    jobs += [(src_in, src), (wide_in, wide), (tab_in.at[TZ:], tab.at[TZ:])]
    copies = [pltpu.make_async_copy(a, b, sems.at[i]) for i, (a, b) in enumerate(jobs)]
    for copy in copies:
        copy.start()
    copies[0].wait()
    row_block = lanes((T, 4 * T), 1) // T % 2
    for i in range(2):
        part = split(jnp.where(row_block == i, tab[4 * H : 4 * H + T, :], 0.0))
        for h in range(2):
            ky[2 * T * h + T * i : 2 * T * h + T * i + T, :] = part[h]
    diagonal = lanes((8, 8 * H), 1) % 8 == lanes((8, 8 * H), 0)
    for t in range(4):
        spread = [jnp.where(diagonal, tab[H * t + j : H * t + j + 1, :], 0.0) for j in range(H)]
        part = split(jnp.concatenate(spread, axis=0))
        for h in range(2):
            if t < 2:
                kx[t, h] = part[h]
            else:
                kxt[t - 2, h] = part[h]
    copies[1].wait()
    eig_row = eig[...]
    for o in range(8):
        base = eig_row + tab[ROWTAB + 8 * o : ROWTAB + 8 * o + 8, NZ : 2 * NZ]
        for p in range(2):
            for j in range(H):
                recip[p, j, 8 * o : 8 * o + 8, :] = 1.0 / (base + float(LAM_T[2 * j + p]))
    mode = lax.axis_index("px") * PY + lax.axis_index("py")
    mu = jnp.sum(jnp.where(lanes((1, NZ), 1) == mode, eig_row, 0.0), axis=1, keepdims=True)
    shift = jnp.concatenate([tab[LAMS : LAMS + 1, :], tab[LAMS + 1 : LAMS + 2, :]], axis=1) + mu
    for i in range(8):
        at = LAMS + 2 + i // 2
        row = tab[at : at + 1, NZ * (i % 2) : NZ * (i % 2) + NZ]
        lam = jnp.broadcast_to(row, (NZ, NZ)).T
        for j in range(4):
            cols = slice(NZ * j, NZ * j + NZ)
            scale[NZ * i : NZ * i + NZ, cols] = 1.0 / (shift[:, cols] + lam)
    copies[2].wait()
    copies[3].wait()
    mass_col = jnp.broadcast_to(mass[...], (NZ, NZ)).T
    w = vertical_table(mass_col * modes[...])
    copies[4].wait()
    mods = [[], []]
    for g in range(8):
        near = src[4 * g : 4 * g + 4].reshape(4 * T, NZ)
        far = jnp.concatenate([src[63 - 4 * g - i] for i in range(4)], axis=0)
        mods[0].append(vertical(near + far, w))
        mods[1].append(vertical(near - far, w))
    table = ky[...]
    for p in range(2):
        for g in range(8):
            res = along_y(table, mods[p][g])
            for i in range(2):
                part = res[:, i * NZ : i * NZ + NZ].reshape(2, T, NZ)
                ybuf[4 * g + 2 * i : 4 * g + 2 * i + 2, :, p * NZ : p * NZ + NZ] = part
    across = [[None] * 8, [None] * 8]
    along = []
    for p in range(2):
        kxp = two(kx, p)
        acc_y = [None] * H
        for q in range(4):
            parts = [
                ybuf[:, 8 * o : 8 * o + 8, p * NZ : (p + 1) * NZ].reshape(8 * H, NZ)
                for o in (2 * q, 2 * q + 1)
            ]
            spec = dot3(kxp, split(jnp.concatenate(parts, axis=1)))
            for i in range(2):
                o = 2 * q + i
                block = spec[:, i * NZ : (i + 1) * NZ]
                coef[p, :, 8 * o : 8 * o + 8, :] = block.reshape(H, 8, NZ)
                edge_b = tab[ROWTAB + 8 * o : ROWTAB + 8 * o + 8, 0:NZ]
                acc_x = None
                for j in range(H):
                    v = block[8 * j : 8 * j + 8] * recip[p, j, 8 * o : 8 * o + 8, :]
                    vx = v * float(EDGE[2 * j + p])
                    vy = v * edge_b
                    acc_x = vx if acc_x is None else acc_x + vx
                    acc_y[j] = vy if acc_y[j] is None else acc_y[j] + vy
                across[p][o] = acc_x
        along.append(jnp.concatenate(acc_y, axis=0))
    copies[5].wait()
    copies[6].wait()
    even = jnp.concatenate(across[0], axis=0)
    odd = jnp.concatenate(across[1], axis=0)
    sums = split(jnp.concatenate(along, axis=1))
    sel = wide[YSEL : YSEL + T, :]
    ends = dot(sel, sums[0]) + dot(sel, sums[1])
    first = jnp.concatenate([ends[:H, :NZ], ends[:H, NZ:]], axis=0)
    last = jnp.concatenate([ends[H:, :NZ], ends[H:, NZ:]], axis=0)
    xs = jnp.concatenate([even + odd, even - odd], axis=0)
    ys = jnp.concatenate([first, last], axis=0)
    edges[pl.ds(0, NZ, stride=2), :] = xs.T
    edges[pl.ds(1, NZ, stride=2), :] = ys.T


def turned(m):
    return jnp.concatenate([m[PY * (PX - 1 - i) : PY * (PX - i)] for i in range(PX)], axis=0)


def swap(m):
    return pltpu.roll(m, T, 1)


def interface_kernel(got, tab, wide, scale, out, xbuf):
    block = lambda at: wide[at : at + 256, :]
    cyl = [(block(CYL + 512 * i), block(CYL + 512 * i + 256)) for i in range(2)]
    lane = lanes((NZ, NZ), 1)
    low = lane < T
    low32 = low[: 2 * PX]
    low16 = low[:PX]
    low64 = low[:T]
    sign_b = jnp.where(lanes((2 * PX, NZ), 1) % 2 == 0, 1.0, -1.0)
    sign_a = jnp.where(lanes((T, NZ), 1) % T < H, 1.0, -1.0)
    gx = got[pl.ds(0, NZ, stride=2), :]
    gy = got[pl.ds(1, NZ, stride=2), :]

    mirror = swap(turned(gx))
    xbuf[...] = jnp.where(low, gx + mirror, swap(gx - mirror))
    tiles = []
    for q in range(4):
        rows = []
        for i in range(2):
            d = xbuf[pl.ds(2 * q + i, PX, stride=PY), :]
            other = swap(d)
            rows.append(jnp.concatenate([d, other] if i == 0 else [other, d], axis=0))
        tiles.append(jnp.where(low32, rows[0], rows[1]))
    flipped = [sign_b * swap(tiles[3 - q]) for q in range(2)]
    line_e = jnp.concatenate([tiles[q] + flipped[q] for q in range(2)], axis=1)
    line_o = jnp.concatenate([tiles[q] - flipped[q] for q in range(2)], axis=1)
    t1 = jnp.concatenate(
        [dot3(split(line_e), cyl[0]), dot3(split(line_o), cyl[1])], axis=1
    )
    t1h, t1l = split(t1)

    back = turned(gy)[:T]
    part_e = gy[:T] + sign_a * back
    part_o = gy[:T] - sign_a * back
    ends = jnp.concatenate(
        [jnp.where(low64, part_e, swap(part_o)), jnp.where(low64, swap(part_e), part_o)], axis=0
    ).T
    by_h, by_l = [
        jnp.concatenate([wide[at : at + NZ, :], wide[at + NZ : at + 2 * NZ, :]], axis=1)
        for at in (BYS, BYS + 256)
    ]
    by_lh = jnp.concatenate([by_l, by_h], axis=0)
    by_hl = jnp.concatenate([by_h, by_l], axis=0)
    chunks = [(p, c) for p in range(2) for c in range(2)]
    m = [block(M12 + 512 * p + 256 * c) for p, c in chunks]
    starts = []
    weights = []
    pad = jnp.zeros((NZ - 3 * PX, NY), BF16)
    for p in range(2):
        e = split(ends[T * p : T * p + T])
        eh, el = block_diag2(e[0]), block_diag2(e[1])
        starts.append((jnp.concatenate([eh, eh], axis=0), el))
        th, tl = t1h[PX * p : PX * p + PX], t1l[PX * p : PX * p + PX]
        weights.append(jnp.concatenate([by_h, th, th, tl, pad], axis=0))
    turns = [
        [
            jnp.concatenate([tab[TR + NZ * p : TR + NZ * p + NZ, NZ * j : NZ * j + NZ]] * 2, axis=1)
            for j in range(2)
        ]
        for p in range(2)
    ]
    zs, us, bxs, rs, bys = {}, {}, {}, {}, {}

    def enter(i):
        p, c = chunks[i]
        zz = dot(m[i], starts[p][0]) + dot(m[i][:, :NZ], starts[p][1])
        turn = tab[TZ + 16 * p : TZ + 16 * p + 16, :][None]
        zz = (zz.reshape(16, 16, 256) * turn).reshape(256, 256)
        zs[i] = split(zz[:, :NZ] + zz[:, NZ:])

    def scaled(i):
        p, c = chunks[i]
        zh, zl = zs[i]
        bk = wide[BKX + 256 * p : BKX + 256 * p + 256, NZ * c : NZ * c + NZ]
        spec = dot(jnp.concatenate([zh, zl], axis=1), by_lh)
        spec += dot(jnp.concatenate([zh, bk], axis=1), weights[p])
        us[i] = split(spec * scale[512 * p + 256 * c : 512 * p + 256 * c + 256, :])

    def lines_of(i):
        p, c = chunks[i]
        at = [BKXT + 64 * p + 32 * h + 16 * c for h in range(2)]
        lines = jnp.concatenate([wide[k : k + 16, :] for k in at], axis=0)
        bxs[i] = halves(dot(lines, us[i][0]), 0) + dot(lines[:16], us[i][1])

    def rows_of(i):
        p, c = chunks[i]
        r = halves(dot(by_hl, us[i][0], NT), 0) + dot(by_h, us[i][1], NT)
        rs[i] = split(jnp.concatenate([r * turns[p][0], r * turns[p][1]], axis=0))

    def leave(i):
        rh, rl = rs[i]
        both = dot(rh, m[i])
        bys[i] = both[:, :NZ] + both[:, NZ:] + dot(rl, m[i][:, :NZ])

    enter(0)
    enter(1)
    enter(2)
    enter(3)
    scaled(0)
    scaled(1)
    rows_of(0)
    lines_of(0)
    scaled(2)
    rows_of(1)
    lines_of(1)
    scaled(3)
    rows_of(2)
    lines_of(2)
    rows_of(3)
    lines_of(3)
    leave(0)
    leave(1)
    leave(2)
    leave(3)
    back_x = [bxs[0] + bxs[1], bxs[2] + bxs[3]]
    back_y = [bys[0] + bys[1], bys[2] + bys[3]]
    back_y = [y[:NZ] + swap(y[NZ:]) for y in back_y]

    bx = jnp.concatenate(back_x, axis=0)
    we = dot3(split(bx[:, : NY // 2]), cyl[0], NT)
    wo = dot3(split(bx[:, NY // 2 :]), cyl[1], NT)
    near = we + wo
    far = we - wo
    for q in range(4):
        if q < 2:
            t = near[:, q * NZ : (q + 1) * NZ]
        else:
            t = swap(sign_b * far[:, (3 - q) * NZ : (4 - q) * NZ])
        s0 = t[:PX] + t[PX:]
        s1 = t[:PX] - t[PX:]
        xbuf[pl.ds(2 * q, PX, stride=PY), :] = jnp.where(low16, s0, swap(s1))
        xbuf[pl.ds(2 * q + 1, PX, stride=PY), :] = jnp.where(low16, swap(s0), s1)
    w = xbuf[...]
    other = swap(gx)
    own = jnp.where(
        low,
        jnp.concatenate([gx[:PY], other[:-PY]], axis=0),
        jnp.concatenate([other[PY:], gx[-PY:]], axis=0),
    )
    out[pl.ds(0, NZ, stride=2), :] = jnp.where(low, w, turned(w)) + own

    near = back_y[0] + back_y[1]
    far = back_y[0] - back_y[1]
    near = jnp.where(low64, near[:T], swap(near[T:]))
    far = sign_a * jnp.where(low64, far[:T], swap(far[T:]))
    w = jnp.concatenate([near, turned(jnp.concatenate([far, far], axis=0))[:T]], axis=0)
    row = lanes((NZ, NZ), 0) % PY
    other = swap(gy)
    own = jnp.where(
        low,
        jnp.where(row == 0, gy, pltpu.roll(other, 1, 0)),
        jnp.where(row == PY - 1, gy, pltpu.roll(other, NZ - 1, 0)),
    )
    out[pl.ds(1, NZ, stride=2), :] = w + own


def backward_kernel(coef, recip, got, modes, ky, kxt, tab, dest, ybuf, qbuf, obuf, sems):
    qbuf[0:NZ] = got[pl.ds(0, NZ, stride=2), :].T
    qbuf[NZ : 2 * NZ] = got[pl.ds(1, NZ, stride=2), :].T
    sign = jnp.where(lanes((8, NZ), 0) % 2 == 0, 1.0, -1.0)
    w = vertical_table(modes[...].T)
    for p in range(2):
        kxp = two(kxt, p)
        ends = []
        for j in range(H):
            at = NZ + p * H + j
            ends.append(qbuf[at : at + 1] + sign * qbuf[at + T : at + T + 1])
        for q in range(4):
            parts = []
            for o in (2 * q, 2 * q + 1):
                near = qbuf[8 * o : 8 * o + 8]
                far = qbuf[T + 8 * o : T + 8 * o + 8]
                line = near + far if p == 0 else near - far
                edge_b = tab[ROWTAB + 8 * o : ROWTAB + 8 * o + 8, 0:NZ]
                blocks = []
                for j in range(H):
                    edge = line * float(EDGE[2 * j + p]) + ends[j] * edge_b
                    r = coef[p, j, 8 * o : 8 * o + 8, :] + edge
                    blocks.append(r * recip[p, j, 8 * o : 8 * o + 8, :])
                parts.append(jnp.concatenate(blocks, axis=0))
            back = dot3(kxp, split(jnp.concatenate(parts, axis=1)))
            for i in range(2):
                o = 2 * q + i
                ybuf[:, 8 * o : 8 * o + 8, p * NZ : (p + 1) * NZ] = back[
                    :, i * NZ : (i + 1) * NZ
                ].reshape(H, 8, NZ)
    table = ky[...]
    copies = []
    for g in range(8):
        outs = []
        for p in range(2):
            block = ybuf[4 * g : 4 * g + 4, :, p * NZ : p * NZ + NZ].reshape(4 * T, NZ)
            res = along_y(table, block)
            outs.append(vertical(jnp.concatenate([res[:, :NZ], res[:, NZ:]], axis=0), w))
        even, odd = outs
        obuf[4 * g : 4 * g + 4] = (even + odd).reshape(4, T, NZ)
        other = even - odd
        for i in range(4):
            obuf[63 - 4 * g - i] = other[T * i : T * i + T]
        for lo, hi in SENDS.get(g, ()):
            i = len(copies)
            copies.append(pltpu.make_async_copy(obuf.at[lo:hi], dest.at[lo:hi], sems.at[i]))
            copies[i].start()
    for copy in copies:
        copy.wait()


SENDS = {3: ((0, 16), (48, 64)), 5: ((16, 24), (40, 48)), 7: ((24, 40),)}
VMEM = pl.BlockSpec(memory_space=pltpu.VMEM)
HBM = pl.BlockSpec(memory_space=pltpu.HBM)
INTERPRET = False


def like(array):
    return jax.ShapeDtypeStruct(array.shape, array.dtype)


def exchange(value):
    value = value.reshape(NZ, 1, 2 * NZ)
    value = lax.all_to_all(value, AXES, split_axis=0, concat_axis=0, tiled=True)
    return value.reshape(2 * NZ, NZ)


def shards(source, layer_mass, modes, mode_eigen):
    tab, wide = solve_tables()
    params = pltpu.CompilerParams(vmem_limit_bytes=40 * 1024 * 1024)
    eig = mode_eigen[None]
    mass = layer_mass[None]
    edge_shape = jax.ShapeDtypeStruct((2 * NZ, NZ), F32)
    field = jax.ShapeDtypeStruct((2, H, T, NZ), F32)
    kron = (2, 8 * H, 8 * H)
    operands = [
        pltpu.with_memory_space_constraint(jnp.asarray(v), pltpu.HBM)
        for v in (source, mass, modes, eig, tab, wide)
    ]
    coef, recip, edges, ky, kxt, modes, tab, wide, scale = pl.pallas_call(
        forward_kernel,
        out_shape=(
            field,
            field,
            edge_shape,
            jax.ShapeDtypeStruct(kron[1:], BF16),
            jax.ShapeDtypeStruct((2, *kron), BF16),
            like(modes),
            like(tab),
            like(wide),
            jax.ShapeDtypeStruct((NX, NY), F32),
        ),
        in_specs=[HBM] * 6,
        out_specs=[VMEM] * 9,
        scratch_shapes=[
            pltpu.VMEM((T, T, NZ), F32),
            pltpu.VMEM((1, NZ), F32),
            pltpu.VMEM((1, NZ), F32),
            pltpu.VMEM((2, *kron), BF16),
            pltpu.VMEM((H, T, 2 * NZ), F32),
            pltpu.SemaphoreType.DMA((7,)),
        ],
        compiler_params=params,
        interpret=INTERPRET,
        name="forward",
    )(*operands)
    values = pl.pallas_call(
        interface_kernel,
        out_shape=edge_shape,
        in_specs=[VMEM] * 4,
        out_specs=VMEM,
        scratch_shapes=[pltpu.VMEM((NZ, NZ), F32)],
        compiler_params=params,
        interpret=INTERPRET,
        name="interface",
    )(exchange(edges), tab, wide, scale)
    return pl.pallas_call(
        backward_kernel,
        out_shape=jax.ShapeDtypeStruct((T, T, NZ), F32),
        in_specs=[VMEM] * 7,
        out_specs=HBM,
        scratch_shapes=[
            pltpu.VMEM((H, T, 2 * NZ), F32),
            pltpu.VMEM((2 * NZ, NZ), F32),
            pltpu.VMEM((T, T, NZ), F32),
            pltpu.SemaphoreType.DMA((5,)),
        ],
        compiler_params=params,
        interpret=INTERPRET,
        name="backward",
    )(coef, recip, exchange(values), modes, ky, kxt, tab)


def solution(mesh):
    placed = (P("px", "py", None), P(), P(), P())
    return jax.shard_map(
        shards, mesh=mesh, in_specs=placed, out_specs=P("px", "py", None), check_vma=False
    )
```

```python
import jax
import jax.numpy as jnp
import numpy as np
from jax import lax
from jax.experimental import pallas as pl
from jax.experimental.pallas import tpu as pltpu
from jax.sharding import PartitionSpec as P

NX, NY, NZ = 1024, 512, 128
PX, PY = 16, 8
T = 64
H = T // 2
F32 = jnp.float32
BF16 = jnp.bfloat16
AXES = ("px", "py")


def np_split(table):
    table = np.asarray(table, np.float64)
    high = table.astype(np.float32).astype(jnp.bfloat16)
    low = (table - high.astype(np.float64)).astype(np.float32).astype(jnp.bfloat16)
    return high, low


def pair(table):
    return np.stack(np_split(table))


def sine_table():
    a = np.arange(1, T + 1)
    return np.sqrt(2.0 / (T + 1)) * np.sin(np.pi * np.outer(a, a) / (T + 1))


SINE = sine_table()
EDGE = SINE[:, 0]
LAM_T = 2.0 - 2.0 * np.cos(np.pi * np.arange(1, T + 1) / (T + 1))
ORDER_A = np.concatenate([np.arange(0, T, 2), np.arange(1, T, 2)])


def norm_row(length):
    return np.where(np.arange(length) == 0, np.sqrt(1.0 / length), np.sqrt(2.0 / length))


def tile_tables():
    rows = [SINE[p::2, :H] for p in range(2)] + [SINE[p::2, :H].T for p in range(2)]
    spread = np.concatenate([np.repeat(r, 8, axis=1) for r in rows])
    small = np.concatenate([spread, np.tile(SINE, (1, 4))]).astype(np.float32)
    edge_b = np.broadcast_to(EDGE[:, None], (T, NZ))
    lam_b = np.broadcast_to(LAM_T[:, None], (T, NZ))
    rowtab = np.concatenate([edge_b, lam_b], axis=1).astype(np.float32)
    signs = np.stack([np.ones(8), (-1.0) ** np.arange(8)])
    ysel = np.concatenate([np.kron(np.eye(H), signs[s : s + 1]) for s in range(2)])
    return small, rowtab, ysel.astype(jnp.bfloat16)


def solve_tables():
    al, be = np.arange(NX), np.arange(NY)
    sx, sy = norm_row(NX), norm_row(NY)
    by_parity = lambda n: np.concatenate([np.arange(0, n, 2), np.arange(1, n, 2)])
    al, be = by_parity(NX), by_parity(NY)
    sx, sy = sx[al], sy[be]
    local = np.arange(T) + 0.5
    lines_x = T * np.arange(PX) - 0.5
    lines_y = np.stack([T * np.arange(PY) - 0.5, T * np.arange(PY) + T + 0.5])
    bkx = sx[:, None] * np.cos(np.pi * al[:, None] * lines_x[None] / NX)
    bky = sy[:, None] * np.cos(np.pi * be[:, None] * lines_y.reshape(1, -1) / NY)
    bky = bky.reshape(NY, 2, 1, PY)
    bys = np.broadcast_to(bky, (NY, 2, PX // 2, PY)).reshape(NY, PX * PY).T
    place = np.arange(NY // 2) + 0.5
    cy = sy[:, None] * np.cos(np.pi * be[:, None] * place[None] / NY)
    cyl = np.einsum("bpy,cy->pcb", cy.reshape(NY, PY // 2, T), SINE).reshape(NY // 2, NY)
    cyl = np.stack([pair(cyl[:, : NY // 2]), pair(cyl[:, NY // 2 :])])
    phase = np.pi * al[:, None] * local[None] / NX
    m1 = (sx[:, None] * np.cos(phase)) @ SINE[:, ORDER_A]
    m2 = (sx[:, None] * np.sin(phase)) @ SINE[:, ORDER_A]
    m12 = np.concatenate(np_split(np.concatenate([m1, m2], axis=1)), axis=1)
    lam_x = 2.0 - 2.0 * np.cos(np.pi * al / NX)
    bkx_h, bkx_l = np_split(bkx)
    bkx_all = np.zeros((NX, 128), jnp.bfloat16)
    for i, part in enumerate((bkx_h, bkx_l, bkx_h)):
        bkx_all[:, 16 * i : 16 * i + part.shape[1]] = part
    bkxt = np.stack([pair(bkx[512 * p : 512 * p + 512].T) for p in range(2)])
    px = np.arange(PX // 2)
    tz, tr = [], []
    for p in range(2):
        turn = np.pi * (2 * np.arange(16) + p)[:, None] * px[None] / PX
        wide = [np.tile(np.repeat(t, PY, axis=1), (1, 2)) for t in (np.cos(turn), -np.sin(turn))]
        tz.append(np.concatenate(wide, axis=1))
        tr += [np.tile(t.T, (1, 8)) for t in wide]
    tz = np.concatenate(tz).astype(np.float32)
    tr = np.stack(tr).astype(np.float32)
    lam_y = (2.0 - 2.0 * np.cos(np.pi * be / NY)).astype(np.float32)[None]
    bys = pair(bys)
    bys = np.concatenate([bys[:, :, :256], bys[:, :, 256:]], axis=1)
    bkx_all = bkx_all.reshape(2, 2, 256, 128)
    bkx_all = np.concatenate([bkx_all[:, 0], bkx_all[:, 1]], axis=2)
    bkxt = bkxt.reshape(2, 2, 16, 2, 256).transpose(0, 1, 3, 2, 4)
    tr = np.stack([np.concatenate([tr[2 * p], tr[2 * p + 1]], axis=1) for p in range(2)])
    small, rowtab, ysel = tile_tables()
    lams = [lam_y.reshape(2, 256), lam_x.astype(np.float32).reshape(4, 256)]
    lams = np.concatenate([*lams, np.zeros((2, 256), np.float32)])
    flat = lambda parts: np.concatenate([t.reshape(-1, 256) for t in parts])
    return flat([small, rowtab, lams, tz, tr]), flat([cyl, m12, bkx_all, bys, bkxt, ysel])


SMALL, ROWTAB, LAMS, TZ, TR = 0, 192, 256, 264, 296
CYL, M12, BKX, BYS, BKXT, YSEL = 0, 1024, 2048, 2560, 3072, 3200


def split(value):
    high = value.astype(BF16)
    return high, (value - high.astype(F32)).astype(BF16)


PLAIN = (((1,), (0,)), ((), ()))
NT = (((1,), (1,)), ((), ()))


def dot(a, b, dims=PLAIN):
    return lax.dot_general(a, b, dims, preferred_element_type=F32)


def dot3(a, b, dims=PLAIN):
    return dot(a[0], b[0], dims) + dot(a[0], b[1], dims) + dot(a[1], b[0], dims)


def halves(value, axis):
    size = value.shape[axis] // 2
    if axis == 0:
        return value[:size] + value[size:]
    return value[:, :size] + value[:, size:]


def vertical(rows, w):
    return halves(dot(jnp.concatenate(split(rows), axis=1), w), 1)


def vertical_table(w):
    both = jnp.concatenate(split(w), axis=1)
    return jnp.concatenate([both, both], axis=0)


def along_y(table, block):
    both = jnp.concatenate([block[: 2 * T], block[2 * T :]], axis=1)
    return halves(dot(table, jnp.concatenate(split(both), axis=0)), 0)


def block_diag2(w):
    zero = jnp.zeros_like(w)
    top = jnp.concatenate([w, zero], axis=1)
    bottom = jnp.concatenate([zero, w], axis=1)
    return jnp.concatenate([top, bottom], axis=0)


def two(ref, *index):
    return ref[(*index, 0)], ref[(*index, 1)]


def lanes(shape, axis):
    return lax.broadcasted_iota(jnp.int32, shape, axis)


def forward_kernel(
    src_in, mass_in, modes_in, eig_in, tab_in, wide_in,
    coef, recip, edges, ky, kxt, modes, tab, wide, scale,
    src, mass, eig, kx, ybuf, sems,
):
    jobs = [(tab_in.at[:TZ], tab.at[:TZ]), (eig_in, eig), (mass_in, mass), (modes_in, modes)]
    jobs += [(src_in, src), (wide_in, wide), (tab_in.at[TZ:], tab.at[TZ:])]
    copies = [pltpu.make_async_copy(a, b, sems.at[i]) for i, (a, b) in enumerate(jobs)]
    for copy in copies:
        copy.start()
    copies[0].wait()
    row_block = lanes((T, 4 * T), 1) // T % 2
    for i in range(2):
        part = split(jnp.where(row_block == i, tab[4 * H : 4 * H + T, :], 0.0))
        for h in range(2):
            ky[2 * T * h + T * i : 2 * T * h + T * i + T, :] = part[h]
    diagonal = lanes((8, 8 * H), 1) % 8 == lanes((8, 8 * H), 0)
    for t in range(4):
        spread = [jnp.where(diagonal, tab[H * t + j : H * t + j + 1, :], 0.0) for j in range(H)]
        part = split(jnp.concatenate(spread, axis=0))
        for h in range(2):
            if t < 2:
                kx[t, h] = part[h]
            else:
                kxt[t - 2, h] = part[h]
    copies[1].wait()
    eig_row = eig[...]
    for o in range(8):
        base = eig_row + tab[ROWTAB + 8 * o : ROWTAB + 8 * o + 8, NZ : 2 * NZ]
        for p in range(2):
            for j in range(H):
                recip[p, j, 8 * o : 8 * o + 8, :] = 1.0 / (base + float(LAM_T[2 * j + p]))
    mode = lax.axis_index("px") * PY + lax.axis_index("py")
    mu = jnp.sum(jnp.where(lanes((1, NZ), 1) == mode, eig_row, 0.0), axis=1, keepdims=True)
    shift = jnp.concatenate([tab[LAMS : LAMS + 1, :], tab[LAMS + 1 : LAMS + 2, :]], axis=1) + mu
    for i in range(8):
        at = LAMS + 2 + i // 2
        row = tab[at : at + 1, NZ * (i % 2) : NZ * (i % 2) + NZ]
        lam = jnp.broadcast_to(row, (NZ, NZ)).T
        for j in range(4):
            cols = slice(NZ * j, NZ * j + NZ)
            scale[NZ * i : NZ * i + NZ, cols] = 1.0 / (shift[:, cols] + lam)
    copies[2].wait()
    copies[3].wait()
    mass_col = jnp.broadcast_to(mass[...], (NZ, NZ)).T
    w = vertical_table(mass_col * modes[...])
    copies[4].wait()
    mods = [[], []]
    for g in range(8):
        near = src[4 * g : 4 * g + 4].reshape(4 * T, NZ)
        far = jnp.concatenate([src[63 - 4 * g - i] for i in range(4)], axis=0)
        mods[0].append(vertical(near + far, w))
        mods[1].append(vertical(near - far, w))
    table = ky[...]
    for p in range(2):
        for g in range(8):
            res = along_y(table, mods[p][g])
            for i in range(2):
                part = res[:, i * NZ : i * NZ + NZ].reshape(2, T, NZ)
                ybuf[4 * g + 2 * i : 4 * g + 2 * i + 2, :, p * NZ : p * NZ + NZ] = part
    across = [[None] * 8, [None] * 8]
    along = []
    for p in range(2):
        kxp = two(kx, p)
        acc_y = [None] * H
        for q in range(4):
            parts = [
                ybuf[:, 8 * o : 8 * o + 8, p * NZ : (p + 1) * NZ].reshape(8 * H, NZ)
                for o in (2 * q, 2 * q + 1)
            ]
            spec = dot3(kxp, split(jnp.concatenate(parts, axis=1)))
            for i in range(2):
                o = 2 * q + i
                block = spec[:, i * NZ : (i + 1) * NZ]
                coef[p, :, 8 * o : 8 * o + 8, :] = block.reshape(H, 8, NZ)
                edge_b = tab[ROWTAB + 8 * o : ROWTAB + 8 * o + 8, 0:NZ]
                acc_x = None
                for j in range(H):
                    v = block[8 * j : 8 * j + 8] * recip[p, j, 8 * o : 8 * o + 8, :]
                    vx = v * float(EDGE[2 * j + p])
                    vy = v * edge_b
                    acc_x = vx if acc_x is None else acc_x + vx
                    acc_y[j] = vy if acc_y[j] is None else acc_y[j] + vy
                across[p][o] = acc_x
        along.append(jnp.concatenate(acc_y, axis=0))
    copies[5].wait()
    copies[6].wait()
    even = jnp.concatenate(across[0], axis=0)
    odd = jnp.concatenate(across[1], axis=0)
    sums = split(jnp.concatenate(along, axis=1))
    sel = wide[YSEL : YSEL + T, :]
    ends = dot(sel, sums[0]) + dot(sel, sums[1])
    first = jnp.concatenate([ends[:H, :NZ], ends[:H, NZ:]], axis=0)
    last = jnp.concatenate([ends[H:, :NZ], ends[H:, NZ:]], axis=0)
    xs = jnp.concatenate([even + odd, even - odd], axis=0)
    ys = jnp.concatenate([first, last], axis=0)
    edges[pl.ds(0, NZ, stride=2), :] = xs.T
    edges[pl.ds(1, NZ, stride=2), :] = ys.T


def turned(m):
    return jnp.concatenate([m[PY * (PX - 1 - i) : PY * (PX - i)] for i in range(PX)], axis=0)


def swap(m):
    return pltpu.roll(m, T, 1)


PAIRS = ((0, 1), (2, 3), (7, 6), (5, 4))


def interface_kernel(got, tab, wide, scale, out, xbuf):
    block = lambda at: wide[at : at + 256, :]
    cyl = [(block(CYL + 512 * i), block(CYL + 512 * i + 256)) for i in range(2)]
    lane = lanes((NZ, NZ), 1)
    low = lane < T
    low32 = low[: 2 * PX]
    low16 = low[:PX]
    low64 = low[:T]
    sign_b = jnp.where(lanes((2 * PX, NZ), 1) % 2 == 0, 1.0, -1.0)
    sign_a = jnp.where(lanes((T, NZ), 1) % T < H, 1.0, -1.0)
    gx = got[pl.ds(0, NZ, stride=2), :]
    gy = got[pl.ds(1, NZ, stride=2), :]

    swapped_x = swap(gx)
    xbuf[...] = jnp.where(low, gx + turned(swapped_x), swapped_x - turned(gx))
    tiles = []
    for places in PAIRS:
        rows = []
        for i, at in enumerate(places):
            d = xbuf[pl.ds(at, PX, stride=PY), :]
            other = swap(d)
            rows.append(jnp.concatenate([d, other] if i == 0 else [other, d], axis=0))
        tiles.append(jnp.where(low32, rows[0], rows[1]))
    flipped = [sign_b * t for t in tiles[2:]]
    line_e = jnp.concatenate([tiles[q] + flipped[q] for q in range(2)], axis=1)
    line_o = jnp.concatenate([tiles[q] - flipped[q] for q in range(2)], axis=1)
    t1 = jnp.concatenate(
        [dot3(split(line_e), cyl[0]), dot3(split(line_o), cyl[1])], axis=1
    )
    t1h, t1l = split(t1)

    back = turned(gy)[:T]
    part_e = gy[:T] + sign_a * back
    part_o = gy[:T] - sign_a * back
    ends = jnp.concatenate(
        [jnp.where(low64, part_e, swap(part_o)), jnp.where(low64, swap(part_e), part_o)], axis=0
    ).T
    by_h, by_l = [
        jnp.concatenate([wide[at : at + NZ, :], wide[at + NZ : at + 2 * NZ, :]], axis=1)
        for at in (BYS, BYS + 256)
    ]
    by_lh = jnp.concatenate([by_l, by_h], axis=0)
    by_hl = jnp.concatenate([by_h, by_l], axis=0)
    chunks = [(p, c) for p in range(2) for c in range(2)]
    m = [block(M12 + 512 * p + 256 * c) for p, c in chunks]
    starts = []
    weights = []
    pad = jnp.zeros((NZ - 3 * PX, NY), BF16)
    for p in range(2):
        e = split(ends[T * p : T * p + T])
        eh, el = block_diag2(e[0]), block_diag2(e[1])
        starts.append((jnp.concatenate([eh, eh], axis=0), el))
        th, tl = t1h[PX * p : PX * p + PX], t1l[PX * p : PX * p + PX]
        weights.append(jnp.concatenate([by_h, th, th, tl, pad], axis=0))
    turns = [
        [
            jnp.concatenate([tab[TR + NZ * p : TR + NZ * p + NZ, NZ * j : NZ * j + NZ]] * 2, axis=1)
            for j in range(2)
        ]
        for p in range(2)
    ]
    zs, us, bxs, rs, bys = {}, {}, {}, {}, {}

    def enter(i):
        p, c = chunks[i]
        zz = dot(m[i], starts[p][0]) + dot(m[i][:, :NZ], starts[p][1])
        turn = tab[TZ + 16 * p : TZ + 16 * p + 16, :][None]
        zz = (zz.reshape(16, 16, 256) * turn).reshape(256, 256)
        zs[i] = split(zz[:, :NZ] + zz[:, NZ:])

    def scaled(i):
        p, c = chunks[i]
        zh, zl = zs[i]
        bk = wide[BKX + 256 * p : BKX + 256 * p + 256, NZ * c : NZ * c + NZ]
        spec = dot(jnp.concatenate([zh, zl], axis=1), by_lh)
        spec += dot(jnp.concatenate([zh, bk], axis=1), weights[p])
        us[i] = split(spec * scale[512 * p + 256 * c : 512 * p + 256 * c + 256, :])

    def lines_of(i):
        p, c = chunks[i]
        at = [BKXT + 64 * p + 32 * h + 16 * c for h in range(2)]
        lines = jnp.concatenate([wide[k : k + 16, :] for k in at], axis=0)
        bxs[i] = halves(dot(lines, us[i][0]), 0) + dot(lines[:16], us[i][1])

    def rows_of(i):
        p, c = chunks[i]
        r = halves(dot(by_hl, us[i][0], NT), 0) + dot(by_h, us[i][1], NT)
        rs[i] = split(jnp.concatenate([r * turns[p][0], r * turns[p][1]], axis=0))

    def leave(i):
        rh, rl = rs[i]
        both = dot(rh, m[i])
        bys[i] = both[:, :NZ] + both[:, NZ:] + dot(rl, m[i][:, :NZ])

    enter(0)
    enter(1)
    enter(2)
    enter(3)
    scaled(0)
    scaled(1)
    rows_of(0)
    lines_of(0)
    scaled(2)
    rows_of(1)
    lines_of(1)
    scaled(3)
    rows_of(2)
    lines_of(2)
    rows_of(3)
    lines_of(3)
    leave(0)
    leave(1)
    leave(2)
    leave(3)
    back_x = [bxs[0] + bxs[1], bxs[2] + bxs[3]]
    back_y = [bys[0] + bys[1], bys[2] + bys[3]]

    bx = jnp.concatenate(back_x, axis=0)
    we = dot3(split(bx[:, : NY // 2]), cyl[0], NT)
    wo = dot3(split(bx[:, NY // 2 :]), cyl[1], NT)
    near = we + wo
    far = we - wo
    for q, (first, second) in enumerate(PAIRS):
        t = (near if q < 2 else far)[:, q % 2 * NZ : q % 2 * NZ + NZ]
        t = t if q < 2 else sign_b * t
        s0 = t[:PX] + t[PX:]
        s1 = t[:PX] - t[PX:]
        xbuf[pl.ds(first, PX, stride=PY), :] = jnp.where(low16, s0, swap(s1))
        xbuf[pl.ds(second, PX, stride=PY), :] = jnp.where(low16, swap(s0), s1)
    w = xbuf[...]
    other = swapped_x
    own = jnp.where(
        low,
        jnp.concatenate([gx[:PY], other[:-PY]], axis=0),
        jnp.concatenate([other[PY:], gx[-PY:]], axis=0),
    )
    out[pl.ds(0, NZ, stride=2), :] = jnp.where(low, w, turned(w)) + own

    near, far = (
        jnp.where(low64, y[:T] + swap(y[NZ : NZ + T]), swap(y[T:NZ]) + y[NZ + T :])
        for y in (back_y[0] + back_y[1], back_y[0] - back_y[1])
    )
    far = sign_a * far
    w = jnp.concatenate([near, turned(jnp.concatenate([far, far], axis=0))[:T]], axis=0)
    row = lanes((NZ, NZ), 0) % PY
    other = swap(gy)
    own = jnp.where(
        low,
        jnp.where(row == 0, gy, pltpu.roll(other, 1, 0)),
        jnp.where(row == PY - 1, gy, pltpu.roll(other, NZ - 1, 0)),
    )
    out[pl.ds(1, NZ, stride=2), :] = w + own


def backward_kernel(coef, recip, got, modes, ky, kxt, tab, dest, ybuf, qbuf, obuf, sems):
    qbuf[0:NZ] = got[pl.ds(0, NZ, stride=2), :].T
    qbuf[NZ : 2 * NZ] = got[pl.ds(1, NZ, stride=2), :].T
    sign = jnp.where(lanes((8, NZ), 0) % 2 == 0, 1.0, -1.0)
    w = vertical_table(modes[...].T)
    for p in range(2):
        kxp = two(kxt, p)
        ends = []
        for j in range(H):
            at = NZ + p * H + j
            ends.append(qbuf[at : at + 1] + sign * qbuf[at + T : at + T + 1])
        for q in range(4):
            parts = []
            for o in (2 * q, 2 * q + 1):
                near = qbuf[8 * o : 8 * o + 8]
                far = qbuf[T + 8 * o : T + 8 * o + 8]
                line = near + far if p == 0 else near - far
                edge_b = tab[ROWTAB + 8 * o : ROWTAB + 8 * o + 8, 0:NZ]
                blocks = []
                for j in range(H):
                    edge = line * float(EDGE[2 * j + p]) + ends[j] * edge_b
                    r = coef[p, j, 8 * o : 8 * o + 8, :] + edge
                    blocks.append(r * recip[p, j, 8 * o : 8 * o + 8, :])
                parts.append(jnp.concatenate(blocks, axis=0))
            back = dot3(kxp, split(jnp.concatenate(parts, axis=1)))
            for i in range(2):
                o = 2 * q + i
                ybuf[:, 8 * o : 8 * o + 8, p * NZ : (p + 1) * NZ] = back[
                    :, i * NZ : (i + 1) * NZ
                ].reshape(H, 8, NZ)
    table = ky[...]
    copies = []
    for g in range(8):
        outs = []
        for p in range(2):
            block = ybuf[4 * g : 4 * g + 4, :, p * NZ : p * NZ + NZ].reshape(4 * T, NZ)
            res = along_y(table, block)
            outs.append(vertical(jnp.concatenate([res[:, :NZ], res[:, NZ:]], axis=0), w))
        even, odd = outs
        obuf[4 * g : 4 * g + 4] = (even + odd).reshape(4, T, NZ)
        other = even - odd
        for i in range(4):
            obuf[63 - 4 * g - i] = other[T * i : T * i + T]
        for lo, hi in SENDS.get(g, ()):
            i = len(copies)
            copies.append(pltpu.make_async_copy(obuf.at[lo:hi], dest.at[lo:hi], sems.at[i]))
            copies[i].start()
    for copy in copies:
        copy.wait()


SENDS = {3: ((0, 16), (48, 64)), 5: ((16, 24), (40, 48)), 7: ((24, 40),)}
VMEM = pl.BlockSpec(memory_space=pltpu.VMEM)
HBM = pl.BlockSpec(memory_space=pltpu.HBM)
INTERPRET = False


def like(array):
    return jax.ShapeDtypeStruct(array.shape, array.dtype)


def exchange(value):
    value = value.reshape(NZ, 1, 2 * NZ)
    value = lax.all_to_all(value, AXES, split_axis=0, concat_axis=0, tiled=True)
    return value.reshape(2 * NZ, NZ)


def shards(source, layer_mass, modes, mode_eigen):
    tab, wide = solve_tables()
    params = pltpu.CompilerParams(vmem_limit_bytes=40 * 1024 * 1024)
    eig = mode_eigen[None]
    mass = layer_mass[None]
    edge_shape = jax.ShapeDtypeStruct((2 * NZ, NZ), F32)
    field = jax.ShapeDtypeStruct((2, H, T, NZ), F32)
    kron = (2, 8 * H, 8 * H)
    operands = [
        pltpu.with_memory_space_constraint(jnp.asarray(v), pltpu.HBM)
        for v in (source, mass, modes, eig, tab, wide)
    ]
    coef, recip, edges, ky, kxt, modes, tab, wide, scale = pl.pallas_call(
        forward_kernel,
        out_shape=(
            field,
            field,
            edge_shape,
            jax.ShapeDtypeStruct(kron[1:], BF16),
            jax.ShapeDtypeStruct((2, *kron), BF16),
            like(modes),
            like(tab),
            like(wide),
            jax.ShapeDtypeStruct((NX, NY), F32),
        ),
        in_specs=[HBM] * 6,
        out_specs=[VMEM] * 9,
        scratch_shapes=[
            pltpu.VMEM((T, T, NZ), F32),
            pltpu.VMEM((1, NZ), F32),
            pltpu.VMEM((1, NZ), F32),
            pltpu.VMEM((2, *kron), BF16),
            pltpu.VMEM((H, T, 2 * NZ), F32),
            pltpu.SemaphoreType.DMA((7,)),
        ],
        compiler_params=params,
        interpret=INTERPRET,
        name="forward",
    )(*operands)
    values = pl.pallas_call(
        interface_kernel,
        out_shape=edge_shape,
        in_specs=[VMEM] * 4,
        out_specs=VMEM,
        scratch_shapes=[pltpu.VMEM((NZ, NZ), F32)],
        compiler_params=params,
        interpret=INTERPRET,
        name="interface",
    )(exchange(edges), tab, wide, scale)
    return pl.pallas_call(
        backward_kernel,
        out_shape=jax.ShapeDtypeStruct((T, T, NZ), F32),
        in_specs=[VMEM] * 7,
        out_specs=HBM,
        scratch_shapes=[
            pltpu.VMEM((H, T, 2 * NZ), F32),
            pltpu.VMEM((2 * NZ, NZ), F32),
            pltpu.VMEM((T, T, NZ), F32),
            pltpu.SemaphoreType.DMA((5,)),
        ],
        compiler_params=params,
        interpret=INTERPRET,
        name="backward",
    )(coef, recip, exchange(values), modes, ky, kxt, tab)


def solution(mesh):
    placed = (P("px", "py", None), P(), P(), P())
    return jax.shard_map(
        shards, mesh=mesh, in_specs=placed, out_specs=P("px", "py", None), check_vma=False
    )
```
